32 devices in a mesh: gx: 8 (over z, y), gy: 4 (over x, core).
Axes of the slice: x: 2, y: 2, z: 4, core: 2. Of those that a mesh axis runs over, the one named last changes fastest.
Arguments:
- anomalies: float32 [80, 16, 32, 128], P(None, 'gx', 'gy'), may hold values from -6 to 6
- state_mean: float32 [16, 32, 128], P('gx', 'gy'), may hold values from -6 to 6
- obs_value: float32 [16, 256], P(None, 'gy'), may hold values from -8 to 8
- obs_cell: int32 [16, 256], replicated, may hold values from 0 to 2047
- owner: int32 [16], replicated, may hold values from 0 to 7, as said below
- order: int32 [16], replicated, may hold values from 0 to 15, each once
- root_inv: float32 [16, 256, 256], P(None, 'gy'), as said below
- gain_inv: float32 [16, 256, 256], P(None, 'gy'), as said below
Outputs:
- post_anomalies: float32 [80, 16, 32, 128], P(None, 'gx', 'gy')
- post_mean: float32 [16, 32, 128], P('gx', 'gy')
The draws below stay inside these ranges and needn't reach their ends.
Inputs may be any that keep to these rules, and one draw needn't show every extreme that they name: `owner`: some batch lies at slab 8 - 2, some at slab 1 and some at slab 8 // 2; the others favour low slabs. `order`: each batch number once. `root_inv`: symmetric. `gain_inv`: symmetric.
All inputs are finite; a program needn't handle non-finite values.
Results may differ from the reference program's by a relative error of at most 0.0001.
Values sent between devices are 32-bit elements; how exact they have to be, the bound alone decides.
No kernel may reach another device: no remote copies, remote signals or barrier semaphores. Data moves between devices by JAX's collectives and lax.ppermute only.
A program may use at most 64 MiB of HBM per device.

```python
import math
import jax
import jax.numpy as jnp
from jax import lax

MEMBERS = 80
OBS = 256
BATCHES = 16
LON_DEV = 2
LAT_DEV = 8
LEVELS = 128
REACH = 3
NLON = 16
NLAT = 32
CELLS = 2048
N_GX = 8
N_GY = 4


def inverse_table(key, floor_value, top_value):
    key_diag, key_off = jax.random.split(key, 2)
    diagonal = jnp.exp(jax.random.uniform(key_diag, (BATCHES, OBS), jnp.float32, math.log(floor_value), math.log(top_value)))
    spread = 0.6 * math.sqrt(floor_value * top_value) / math.sqrt(OBS)
    offdiag_noise = jax.random.normal(key_off, (BATCHES, OBS, OBS), jnp.float32) * spread
    inverse = 0.5 * (offdiag_noise + jnp.swapaxes(offdiag_noise, 1, 2)) + diagonal[:, :, None] * jnp.eye(OBS, dtype=jnp.float32)
    return inverse


def draw_root_inv(key, part):
    return inverse_table(jax.random.fold_in(key, 11), 0.15, 0.5)


def draw_gain_inv(key, part):
    return inverse_table(jax.random.fold_in(key, 23), 0.3, 0.9)


def draw_owner(key, part):
    key_first, key_second, key_perm = jax.random.split(jax.random.fold_in(key, 37), 3)
    first_draw = jax.random.randint(key_first, (BATCHES,), 0, N_GX, dtype=jnp.int32)
    second_draw = jax.random.randint(key_second, (BATCHES,), 0, N_GX, dtype=jnp.int32)
    slabs = jnp.minimum(first_draw, second_draw)
    anchors = jnp.array([N_GX - 2, 1, N_GX // 2], dtype=jnp.int32)
    slabs = slabs.at[:3].set(anchors)
    shuffle = jax.random.permutation(key_perm, BATCHES)
    return slabs[shuffle].astype(jnp.int32)


def place_ends(drawn, own_key, least, high):
    index_at = [jax.random.randint(jax.random.fold_in(own_key, axis), (), 0, length) for axis, length in enumerate(drawn.shape)]
    longest = drawn.shape.index(max(drawn.shape))
    neighbour = index_at[:longest] + [(index_at[longest] + 1) % drawn.shape[longest]] + index_at[longest + 1:]
    return drawn.at[tuple(index_at)].set(least).at[tuple(neighbour)].set(high)


def block_levels(own_key, shape, cuts, low, largest):
    loudness = 1.0
    for dim, parts in cuts:
        draws = jax.random.uniform(jax.random.fold_in(jax.random.fold_in(own_key, 6), dim), (parts,), jnp.float32, low / len(cuts), largest / len(cuts))
        loudness = loudness * jnp.repeat(jnp.exp(draws), shape[dim] // parts).reshape((-1,) + (1,) * (len(shape) - 1 - dim))
    return loudness


def noise(key, dims, deviation, most, shards=(), kind=jnp.bfloat16):
    level = block_levels(key, dims, shards, -0.22, 0.18) if shards else 1.0
    drawn = jax.random.normal(key, dims, jnp.float32) * deviation * level
    return jnp.minimum(jnp.maximum(drawn, -most), most).astype(kind)


def setup_inputs(seed: int = 0) -> dict:
    arg_keys = jax.random.split(jax.random.key(seed), 9)
    anomalies = noise(arg_keys[0], (MEMBERS, NLON, NLAT, LEVELS), 1.0, 6.0, ((1, 8), (2, 4)), jnp.float32)
    state_mean = noise(arg_keys[1], (NLON, NLAT, LEVELS), 1.0, 6.0, ((0, 8), (1, 4)), jnp.float32)
    obs_value = noise(arg_keys[2], (BATCHES, OBS), 1.5, 8.0, ((1, 4),), jnp.float32)
    obs_cell = place_ends(jax.random.randint(arg_keys[3], (BATCHES, OBS), 0, CELLS), jax.random.fold_in(arg_keys[3], 1), 0, CELLS - 1).astype(jnp.int32)
    owner = draw_owner(jax.random.fold_in(arg_keys[8], 71), 0)
    order = jax.random.permutation(arg_keys[5], BATCHES).astype(jnp.int32)
    root_inv = draw_root_inv(jax.random.fold_in(arg_keys[8], 71), 0)
    gain_inv = draw_gain_inv(jax.random.fold_in(arg_keys[8], 71), 0)
    return {"anomalies": anomalies, "state_mean": state_mean, "obs_value": obs_value, "obs_cell": obs_cell, "owner": owner, "order": order, "root_inv": root_inv, "gain_inv": gain_inv}


def product(left_side, right_side):
    return jnp.dot(left_side, right_side, precision=lax.Precision.HIGHEST, preferred_element_type=jnp.float32)


def reference(anomalies, state_mean, obs_value, obs_cell, owner, order, root_inv, gain_inv):
    lon_total = LON_DEV * N_GX
    lat_total = LAT_DEV * N_GY
    quarter = OBS // N_GY
    window_width = (2 * REACH + 1) * LON_DEV
    reach_cells = REACH * LON_DEV
    taper_span = REACH * LON_DEV + 1.0
    obs_band = jnp.arange(OBS, dtype=jnp.int32) // quarter
    lat_index = jnp.arange(lat_total, dtype=jnp.int32)
    offsets = jnp.arange(window_width, dtype=jnp.int32)

    def assimilate(batch_turn, carried):
        state_field, mean_field = carried
        batch_id = order[batch_turn]
        root_slab = owner[batch_id]
        cells_of = obs_cell[batch_id]
        obs_lon = root_slab * LON_DEV + cells_of // (LAT_DEV * LEVELS)
        obs_lat = obs_band * LAT_DEV + (cells_of // LEVELS) % LAT_DEV
        obs_lev = cells_of % LEVELS
        prior_all = state_field[:, obs_lon, obs_lat, obs_lev]
        innovation = obs_value[batch_id] - mean_field[obs_lon, obs_lat, obs_lev]
        weighted = product(prior_all, root_inv[batch_id].T)
        gain_vec = product(gain_inv[batch_id], innovation)
        window_lon = (root_slab * LON_DEV - reach_cells + offsets) % lon_total
        window = state_field[:, window_lon].reshape(MEMBERS, -1)
        mean_window = mean_field[window_lon].reshape(-1)
        cell_lon = jnp.broadcast_to(window_lon[:, None, None], (window_width, lat_total, LEVELS)).reshape(-1)
        cell_lat = jnp.broadcast_to(lat_index[None, :, None], (window_width, lat_total, LEVELS)).reshape(-1)
        lon_gap = jnp.abs(obs_lon[:, None] - cell_lon[None, :])
        cycle_gap = jnp.minimum(lon_gap, lon_total - lon_gap)
        lat_gap = jnp.abs(obs_lat[:, None] - cell_lat[None, :])
        taper_rows = jnp.maximum(0.0, 1.0 - cycle_gap.astype(jnp.float32) / taper_span) * (1.0 - lat_gap.astype(jnp.float32) / lat_total)
        covariance = product(prior_all.T, window) / (MEMBERS - 1.0)
        gained = taper_rows * covariance
        stacked = jnp.concatenate([weighted, gain_vec[None, :]], axis=0)
        increment = product(stacked, gained)
        new_window = (window - increment[:MEMBERS]).reshape(MEMBERS, window_width, lat_total, LEVELS)
        new_mean = (mean_window + increment[MEMBERS]).reshape(window_width, lat_total, LEVELS)
        state_field = state_field.at[:, window_lon].set(new_window)
        mean_field = mean_field.at[window_lon].set(new_mean)
        return state_field, mean_field

    post_anomalies, post_mean = lax.fori_loop(0, BATCHES, assimilate, (anomalies, state_mean))
    return post_anomalies, post_mean
```

```python
import functools
import jax
import jax.numpy as jnp
from jax import lax
from jax.experimental import pallas as pl
from jax.experimental.pallas import tpu as pltpu
from jax.sharding import PartitionSpec as P

REACH = 3
LANES = 128
CHUNK = 512
F32 = jnp.float32
BF16 = jnp.bfloat16


def swapped(value, axis, mask):
    count = lax.axis_size(axis)
    return lax.ppermute(value, axis, [(source, source ^ mask) for source in range(count)])


def split(value):
    high = value.astype(BF16).astype(F32)
    return high, value - high


def dot(left, right):
    return jnp.dot(left, right, preferred_element_type=F32)


def gather_kernel(
    dims, order, owner, place, cells, anom, mean, obs, own_out, keep_out, send_out, parts
):
    members, blocks, quarter, pairs = dims
    rows = own_out.shape[0]
    column, band = place[0], place[1]
    half = lax.rem(column, 2)
    for k in range(blocks):
        block = anom[pl.ds(k, members, stride=blocks), :]
        extra = jnp.concatenate(
            [-mean[k : k + 1, :], jnp.zeros((rows - members - 1, LANES), F32)], axis=0
        )
        block = jnp.concatenate([block, extra], axis=0)
        own_out[:, k * LANES : (k + 1) * LANES] = block
        high, rest = split(block)
        mid, low = split(rest)
        stack = jnp.concatenate([high, mid, low], axis=0)
        parts[:, k * LANES : (k + 1) * LANES] = stack.astype(BF16)
    lane = lax.broadcasted_iota(jnp.int32, (1, LANES), 1)
    first = lane < quarter
    total = cells.shape[1]
    shift = lax.rem(total - band * quarter, total)

    def ids_of(pair):
        even, odd = order[2 * pair], order[2 * pair + 1]
        row_even = pltpu.roll(cells[pl.ds(even, 1), :], shift, 1)[:, :LANES]
        row_odd = pltpu.roll(cells[pl.ds(odd, 1), :], lax.rem(shift + quarter, total), 1)
        row_odd = row_odd[:, :LANES]
        here_even = owner[even] == column
        here_odd = owner[odd] == column
        mine = jnp.where(first, here_even.astype(jnp.int32), here_odd.astype(jnp.int32))
        ids = jnp.where(mine > 0, jnp.where(first, row_even, row_odd), -1)
        seen = jnp.where(first, obs[pl.ds(even, 1), :], obs[pl.ds(odd, 1), :])
        seen = jnp.where(mine > 0, seen, 0.0)
        return ids, seen, jnp.logical_or(here_even, here_odd)

    for out, which in ((keep_out, half), (send_out, 1 - half)):
        for slot in range(0, pairs // 2, 2):
            pair = which * (pairs // 2) + slot
            ids_a, seen_a, any_a = ids_of(pair)
            ids_b, seen_b, any_b = ids_of(pair + 1)
            ids = jnp.concatenate([ids_a, ids_b], axis=1)
            seen = jnp.concatenate([seen_a, seen_b], axis=1)
            span = slice(slot * LANES, (slot + 2) * LANES)
            busy = jnp.logical_or(any_a, any_b)

            @pl.when(busy)
            def _(out=out, ids=ids, seen=seen, span=span):
                total_cells = parts.shape[1]
                cell = lax.broadcasted_iota(jnp.int32, (total_cells, 2 * LANES), 0)
                hot = jnp.where(cell == ids, 1.0, 0.0).astype(BF16)
                found = dot(parts[...], hot)
                value = found[:rows] + found[rows : 2 * rows] + found[2 * rows :]
                row = lax.broadcasted_iota(jnp.int32, value.shape, 0)
                out[:, span] = value + jnp.where(row == members, seen, 0.0)

            @pl.when(jnp.logical_not(busy))
            def _(out=out, span=span):
                out[:, span] = jnp.zeros((rows, 2 * LANES), F32)


def chain_kernel(
    dims,
    order,
    owner,
    place,
    cells,
    own,
    *refs,
):
    members, lon_dev, lat_dev, quarter, batches, slabs, bands = dims
    pieces = refs[:8]
    matrices = refs[8:16]
    anom_out, mean_out = refs[16:18]
    state, lon_at, lat_at, near, far, zcat, wcat, lat_of, bit_of, root, gain, sems = refs[18:]
    rows = state.shape[0]
    own_cells = own.shape[1]
    own_tiles = own_cells // LANES
    obs = 4 * quarter
    column, band = place[0], place[1]
    core = lax.rem(band, 2)
    chip = lax.div(band, 2)
    lat_total = float(bands * lat_dev)
    lon_total = float(slabs * lon_dev)
    reach_span = REACH * lon_dev + 1.0

    def loads(turn, slot):
        b = order[turn]
        near_cols = pl.ds(pl.multiple_of(chip * LANES, LANES), LANES)
        far_cols = pl.ds(pl.multiple_of((1 - chip) * LANES, LANES), LANES)
        mine = pl.multiple_of(core * quarter, quarter)
        theirs = pl.multiple_of((1 - core) * quarter, quarter)
        left, right = pl.ds(0, LANES), pl.ds(LANES, LANES)
        found = []
        for kind, buffer in ((0, root), (1, gain)):
            local, partner, across, relayed = matrices[4 * kind : 4 * kind + 4]
            plan = [
                (local.at[b, :, near_cols], mine, left),
                (local.at[b, :, far_cols], mine, right),
                (partner.at[b, :, near_cols], theirs, left),
                (partner.at[b, :, far_cols], theirs, right),
                (across.at[b], 2 * quarter + mine, right),
                (relayed.at[b], 2 * quarter + theirs, right),
            ]
            for source, row, cols in plan:
                sem = sems.at[slot, len(found)]
                target = buffer.at[slot, pl.ds(row, quarter), cols]
                found.append(pltpu.make_async_copy(source, target, sem))
        return found

    for copy in loads(0, 0):
        copy.start()

    state[:, :own_cells] = own[...]
    lane = lax.broadcasted_iota(jnp.int32, (1, LANES), 1)
    first = lane < quarter
    low_core = jnp.where(first, 1, 0) * jnp.where(core == 0, 1, 0) + jnp.where(
        first, 0, 1
    ) * jnp.where(core == 0, 0, 1)
    from_self = low_core > 0
    half_pairs = batches // 4
    half = lax.rem(column, 2)
    for which in range(2):
        pair_base = (half if which == 0 else 1 - half) * half_pairs
        for side in range(2):
            mine = pieces[2 * side + which]
            theirs = pieces[4 + 2 * side + which]
            for k in range(half_pairs):
                span = slice(k * LANES, (k + 1) * LANES)
                a, b = mine[:, span], theirs[:, span]
                a_roll, b_roll = pltpu.roll(a, quarter, 1), pltpu.roll(b, quarter, 1)
                a_first, b_first = (
                    jnp.where(core == 0, a, a_roll),
                    jnp.where(core == 0, b_roll, b),
                )
                a_last, b_last = (
                    jnp.where(core == 0, a_roll, a),
                    jnp.where(core == 0, b, b_roll),
                )
                turn = 2 * (pair_base + k)
                for step, (x, y) in enumerate(((a_first, b_first), (a_last, b_last))):
                    at = own_cells + (batches - 1 - turn - step) * obs + side * LANES
                    at = pl.multiple_of(at, LANES)
                    state[:, pl.ds(at, LANES)] = jnp.where(from_self, x, y)

    tile = lax.broadcasted_iota(jnp.int32, (own_tiles, LANES), 0)
    lon_at[:own_tiles, :] = (column * lon_dev + tile // lat_dev).astype(F32)
    lat_at[:own_tiles, :] = (band * lat_dev + tile % lat_dev).astype(F32) / lat_total

    @pl.loop(0, batches)
    def _(turn):
        b = order[turn]
        cells_row = cells[pl.ds(b, 1), :]
        for side in range(2):
            group = chip if side == 0 else 1 - chip
            cell = jnp.where(group == 0, cells_row[:, :LANES], cells_row[:, LANES:])
            level_band = lax.shift_right_logical(cell, (LANES - 1).bit_length())
            lat = group * 2 + jnp.where(first, 0, 1)
            lat = lat * lat_dev + lax.rem(level_band, lat_dev)
            lon = owner[b] * lon_dev + lax.div(level_band, lat_dev)
            row = own_tiles + (batches - 1 - turn) * 2 + side
            lon_at[pl.ds(row, 1), :] = lon.astype(F32)
            lat_at[pl.ds(row, 1), :] = lat.astype(F32) / lat_total

    @pl.loop(0, batches)
    def _(turn):
        slot = lax.rem(turn, 2)
        for copy in loads(turn, slot):
            copy.wait()

        @pl.when(turn + 1 < batches)
        def _():
            for copy in loads(turn + 1, 1 - slot):
                copy.start()

        slab = owner[order[turn]]

        def factor(lon):
            gap = jnp.abs(lon_at[...] - lon)
            gap = jnp.minimum(gap, lon_total - gap)
            return jnp.maximum(0.0, 1.0 - gap / reach_span)

        base = (slab * lon_dev).astype(F32)
        near[...] = factor(base)
        far[...] = factor(base + 1.0)
        for side in range(2):
            row = own_tiles + (batches - 1 - turn) * 2 + side
            lat_row = jnp.broadcast_to(lat_at[pl.ds(row, 1), :], (LANES, LANES))
            bit_row = jnp.broadcast_to(lon_at[pl.ds(row, 1), :] - base, (LANES, LANES))
            span = slice(side * LANES, (side + 1) * LANES)
            lat_of[span, :] = lat_row.T
            bit_of[span, :] = bit_row.T

        at = pl.multiple_of(own_cells + (batches - 1 - turn) * obs, obs)
        z = state[:, pl.ds(at, obs)]
        z_high, z_low = split(z[:members])
        pad = jnp.zeros((obs - 3 * members, obs), F32)
        zcat[...] = jnp.concatenate([z_high, z_high, z_low, pad], axis=0).T.astype(BF16)
        d_high, d_low = split(z[members:])

        def symmetric(buffer):
            top = buffer[slot, : 2 * quarter, :]
            corner = buffer[slot, 2 * quarter :, 2 * quarter :]
            bottom = jnp.concatenate([top[:, 2 * quarter :].T, corner], axis=1)
            high, low = split(jnp.concatenate([top, bottom], axis=0))
            return high.astype(BF16), low.astype(BF16)

        root_high, root_low = symmetric(root)
        gain_high, gain_low = symmetric(gain)

        def thrice(high, low, right_high, right_low):
            count = high.shape[0]
            both = dot(jnp.concatenate([high, low], axis=0).astype(BF16), right_high)
            return both[:count] + both[count:] + dot(high.astype(BF16), right_low)

        v = thrice(z_high, z_low, root_high, root_low)
        u = thrice(d_high, d_low, gain_high, gain_low)
        w = jnp.concatenate([v, u], axis=0) * (1.0 / (members - 1.0))
        w_high, w_low = split(w)
        wcat[...] = jnp.concatenate([w_high, w_low], axis=0).astype(BF16)

        width = own_cells + (batches - 1 - turn) * obs
        count = lax.div(width + CHUNK - 1, CHUNK)

        @pl.loop(0, count)
        def _(chunk):
            start = pl.multiple_of(chunk * CHUNK, CHUNK)
            now = state[:, pl.ds(start, CHUNK)]
            high, low = split(now[:members])
            zeros = jnp.zeros((obs - 3 * members, CHUNK), F32)
            right = jnp.concatenate([high, low, high, zeros], axis=0).astype(BF16)
            cov = dot(zcat[...], right)
            parts = []
            for k in range(CHUNK // LANES):
                row = chunk * (CHUNK // LANES) + k
                near_row = near[pl.ds(row, 1), :]
                far_row = far[pl.ds(row, 1), :]
                lat_row = lat_at[pl.ds(row, 1), :]
                lat_part = 1.0 - jnp.abs(lat_of[...] - lat_row)
                lon_part = jnp.where(bit_of[...] > 0.5, far_row, near_row)
                parts.append(cov[:, k * LANES : (k + 1) * LANES] * (lat_part * lon_part))
            gained = jnp.concatenate(parts, axis=1)
            g_high = gained.astype(BF16)
            g_low = (gained - g_high.astype(F32)).astype(BF16)
            both = dot(wcat[...], g_high)
            change = both[:rows] + both[rows:] + dot(wcat[:rows, :], g_low)
            state[:, pl.ds(start, CHUNK)] = now - change

    for k in range(own_tiles):
        span = slice(k * LANES, (k + 1) * LANES)
        anom_out[pl.ds(k, members, stride=own_tiles), :] = state[:members, span]
        mean_out[k : k + 1, :] = -state[members : members + 1, span]


def local(anomalies, state_mean, obs_value, obs_cell, owner, order, root_inv, gain_inv):
    members, lon_dev, lat_dev, levels = anomalies.shape
    batches, quarter = obs_value.shape
    obs = obs_cell.shape[1]
    blocks = lon_dev * lat_dev
    own_cells = blocks * levels
    slabs = lax.axis_size("gx")
    bands = lax.axis_size("gy")
    column = lax.axis_index("gx")
    band = lax.axis_index("gy")
    rows = -(-(members + 1) // 8) * 8
    tiles = (own_cells + batches * obs) // LANES
    place = jnp.stack([column, band]).astype(jnp.int32)

    start = lax.div(band, 2) * 2 * quarter
    cut = functools.partial(
        lax.dynamic_slice_in_dim, start_index=start, slice_size=2 * quarter, axis=2
    )
    sent = [cut(root_inv), cut(gain_inv)]
    matrices = [
        [root_inv, swapped(root_inv, "gy", 1), swapped(sent[0], "gy", 2)],
        [gain_inv, swapped(gain_inv, "gy", 1), swapped(sent[1], "gy", 2)],
    ]
    for group in matrices:
        group.append(swapped(group[2], "gy", 1))

    smem = pl.BlockSpec(memory_space=pltpu.SMEM)
    vmem = pl.BlockSpec(memory_space=pltpu.VMEM)
    hbm = pl.BlockSpec(memory_space=pl.ANY)
    pairs = batches // 2
    piece = jax.ShapeDtypeStruct((rows, pairs // 2 * LANES), F32)
    own, keep, send = pl.pallas_call(
        functools.partial(gather_kernel, (members, blocks, quarter, pairs)),
        out_shape=(jax.ShapeDtypeStruct((rows, own_cells), F32), piece, piece),
        in_specs=[smem, smem, smem, vmem, vmem, vmem, vmem],
        out_specs=(vmem, vmem, vmem),
        scratch_shapes=[pltpu.VMEM((3 * rows, own_cells), BF16)],
        name="gather_observations",
    )(
        order,
        owner,
        place,
        obs_cell,
        anomalies.reshape(members * blocks, levels),
        state_mean.reshape(blocks, levels),
        jnp.concatenate([obs_value, obs_value], axis=1),
    )

    mine = keep + swapped(send, "gx", 1)
    mask = 2
    while mask < slabs:
        mine = mine + swapped(mine, "gx", mask)
        mask *= 2
    other = swapped(mine, "gx", 1)
    chip = [mine, other, swapped(mine, "gy", 2), swapped(other, "gy", 2)]
    pieces = chip + [swapped(part, "gy", 1) for part in chip]

    dims = (members, lon_dev, lat_dev, quarter, batches, slabs, bands)
    post, post_mean = pl.pallas_call(
        functools.partial(chain_kernel, dims),
        out_shape=(
            jax.ShapeDtypeStruct((members * blocks, levels), F32),
            jax.ShapeDtypeStruct((blocks, levels), F32),
        ),
        in_specs=[smem, smem, smem] + [vmem] * 10 + [hbm] * 8,
        out_specs=(vmem, vmem),
        scratch_shapes=[
            pltpu.VMEM((rows, own_cells + batches * obs), F32),
            pltpu.VMEM((tiles, LANES), F32),
            pltpu.VMEM((tiles, LANES), F32),
            pltpu.VMEM((tiles, LANES), F32),
            pltpu.VMEM((tiles, LANES), F32),
            pltpu.VMEM((obs, obs), BF16),
            pltpu.VMEM((2 * rows, obs), BF16),
            pltpu.VMEM((obs, LANES), F32),
            pltpu.VMEM((obs, LANES), F32),
            pltpu.VMEM((2, obs, obs), F32),
            pltpu.VMEM((2, obs, obs), F32),
            pltpu.SemaphoreType.DMA((2, 12)),
        ],
        name="observation_recursion",
    )(order, owner, place, obs_cell, own, *pieces, *matrices[0], *matrices[1])
    return (
        post.reshape(members, lon_dev, lat_dev, levels),
        post_mean.reshape(lon_dev, lat_dev, levels),
    )


def solution(mesh):
    return jax.shard_map(
        local,
        mesh=mesh,
        in_specs=(
            P(None, "gx", "gy", None),
            P("gx", "gy", None),
            P(None, "gy"),
            P(),
            P(),
            P(),
            P(None, "gy", None),
            P(None, "gy", None),
        ),
        out_specs=(P(None, "gx", "gy", None), P("gx", "gy", None)),
        check_vma=False,
    )
```

```python
import functools
import jax
import jax.numpy as jnp
from jax import lax
from jax.experimental import pallas as pl
from jax.experimental.pallas import tpu as pltpu
from jax.sharding import PartitionSpec as P

REACH = 3
LANES = 128
CHUNK = 512
GROUP = 4
SLOTS = 4
LAG = 1
HOIST = 32
STRIP = 16
F32 = jnp.float32
BF16 = jnp.bfloat16


def swapped(value, axis, mask):
    count = lax.axis_size(axis)
    return lax.ppermute(value, axis, [(source, source ^ mask) for source in range(count)])


def split(value):
    high = value.astype(BF16).astype(F32)
    return high, value - high


def dot(left, right):
    return jnp.dot(left, right, preferred_element_type=F32)


def gather_kernel(
    dims, order, owner, place, cells, anom, mean, obs, own_out, keep_out, send_out, parts
):
    members, blocks, quarter, pairs = dims
    rows = own_out.shape[0]
    column, band = place[0], place[1]
    half = lax.rem(column, 2)
    for k in range(blocks):
        block = anom[pl.ds(k, members, stride=blocks), :]
        extra = jnp.concatenate(
            [-mean[k : k + 1, :], jnp.zeros((rows - members - 1, LANES), F32)], axis=0
        )
        block = jnp.concatenate([block, extra], axis=0)
        own_out[:, k * LANES : (k + 1) * LANES] = block
        high, rest = split(block)
        mid, low = split(rest)
        stack = jnp.concatenate([high, mid, low], axis=0)
        parts[:, k * LANES : (k + 1) * LANES] = stack.astype(BF16)
    lane = lax.broadcasted_iota(jnp.int32, (1, LANES), 1)
    first = lane < quarter
    total = cells.shape[1]
    shift = lax.rem(total - band * quarter, total)

    def ids_of(pair):
        even, odd = order[2 * pair], order[2 * pair + 1]
        row_even = pltpu.roll(cells[pl.ds(even, 1), :], shift, 1)[:, :LANES]
        row_odd = pltpu.roll(cells[pl.ds(odd, 1), :], lax.rem(shift + quarter, total), 1)
        row_odd = row_odd[:, :LANES]
        here_even = owner[even] == column
        here_odd = owner[odd] == column
        mine = jnp.where(first, here_even.astype(jnp.int32), here_odd.astype(jnp.int32))
        ids = jnp.where(mine > 0, jnp.where(first, row_even, row_odd), -1)
        seen = jnp.where(first, obs[pl.ds(even, 1), :], obs[pl.ds(odd, 1), :])
        seen = jnp.where(mine > 0, seen, 0.0)
        return ids, seen, jnp.logical_or(here_even, here_odd)

    for out, which in ((keep_out, half), (send_out, 1 - half)):
        for slot in range(0, pairs // 2, 2):
            pair = which * (pairs // 2) + slot
            ids_a, seen_a, any_a = ids_of(pair)
            ids_b, seen_b, any_b = ids_of(pair + 1)
            ids = jnp.concatenate([ids_a, ids_b], axis=1)
            seen = jnp.concatenate([seen_a, seen_b], axis=1)
            span = slice(slot * LANES, (slot + 2) * LANES)
            busy = jnp.logical_or(any_a, any_b)

            @pl.when(busy)
            def _(out=out, ids=ids, seen=seen, span=span):
                total_cells = parts.shape[1]
                cell = lax.broadcasted_iota(jnp.int32, (total_cells, 2 * LANES), 0)
                hot = jnp.where(cell == ids, 1.0, 0.0).astype(BF16)
                found = dot(parts[...], hot)
                value = found[:rows] + found[rows : 2 * rows] + found[2 * rows :]
                row = lax.broadcasted_iota(jnp.int32, value.shape, 0)
                out[:, span] = value + jnp.where(row == members, seen, 0.0)

            @pl.when(jnp.logical_not(busy))
            def _(out=out, span=span):
                out[:, span] = jnp.zeros((rows, 2 * LANES), F32)


def chain_kernel(
    dims,
    order,
    owner,
    place,
    cells,
    own,
    *refs,
):
    members, lon_dev, lat_dev, quarter, batches, slabs, bands = dims
    pieces = refs[:8]
    matrices = refs[8:16]
    anom_out, mean_out = refs[16:18]
    state, lon_at, lat_at, slope_at, near, far, zcat, wcat = refs[18:26]
    lat_of, rise_of, bit_of, own_taper, root, gain, sems = refs[26:]
    rows = state.shape[0]
    own_cells = own.shape[1]
    own_tiles = own_cells // LANES
    obs = bands * quarter
    column, band = place[0], place[1]
    core = lax.rem(band, 2)
    chip = lax.div(band, 2)
    lat_total = float(bands * lat_dev)
    lon_total = float(slabs * lon_dev)
    reach_span = REACH * lon_dev + 1.0

    def loads(turn, slot):
        b = order[turn]
        near_cols = pl.ds(pl.multiple_of(chip * LANES, LANES), LANES)
        far_cols = pl.ds(pl.multiple_of((1 - chip) * LANES, LANES), LANES)
        mine = pl.multiple_of(core * quarter, quarter)
        theirs = pl.multiple_of((1 - core) * quarter, quarter)
        left, right = pl.ds(0, LANES), pl.ds(LANES, LANES)
        found = []
        for kind, buffer in ((0, root), (1, gain)):
            local, partner, across, relayed = matrices[4 * kind : 4 * kind + 4]
            plan = [
                (local.at[b, :, near_cols], mine, left),
                (local.at[b, :, far_cols], mine, right),
                (partner.at[b, :, near_cols], theirs, left),
                (partner.at[b, :, far_cols], theirs, right),
                (across.at[b], 2 * quarter + mine, right),
                (relayed.at[b], 2 * quarter + theirs, right),
            ]
            for source, row, cols in plan:
                sem = sems.at[slot, len(found)]
                target = buffer.at[slot, pl.ds(row, quarter), cols]
                found.append(pltpu.make_async_copy(source, target, sem))
        return found

    for copy in loads(0, 0):
        copy.start()

    state[:, :own_cells] = own[...]
    lane = lax.broadcasted_iota(jnp.int32, (1, LANES), 1)
    first = lane < quarter
    low_core = jnp.where(first, 1, 0) * jnp.where(core == 0, 1, 0) + jnp.where(
        first, 0, 1
    ) * jnp.where(core == 0, 0, 1)
    from_self = low_core > 0
    half_pairs = batches // 4
    half = lax.rem(column, 2)
    for which in range(2):
        pair_base = (half if which == 0 else 1 - half) * half_pairs
        for side in range(2):
            mine = pieces[2 * side + which]
            theirs = pieces[4 + 2 * side + which]
            for k in range(half_pairs):
                span = slice(k * LANES, (k + 1) * LANES)
                a, b = mine[:, span], theirs[:, span]
                a_roll, b_roll = pltpu.roll(a, quarter, 1), pltpu.roll(b, quarter, 1)
                a_first, b_first = (
                    jnp.where(core == 0, a, a_roll),
                    jnp.where(core == 0, b_roll, b),
                )
                a_last, b_last = (
                    jnp.where(core == 0, a_roll, a),
                    jnp.where(core == 0, b, b_roll),
                )
                turn = 2 * (pair_base + k)
                for step, (x, y) in enumerate(((a_first, b_first), (a_last, b_last))):
                    at = own_cells + (batches - 1 - turn - step) * obs + side * LANES
                    at = pl.multiple_of(at, LANES)
                    state[:, pl.ds(at, LANES)] = jnp.where(from_self, x, y)

    side_sign = jnp.where(chip > 0, 1.0, -1.0)

    @pl.loop(0, batches)
    def _(turn):
        b = order[turn]
        cells_row = cells[pl.ds(b, 1), :]
        for side in range(2):
            group = chip if side == 0 else 1 - chip
            cell = jnp.where(group == 0, cells_row[:, :LANES], cells_row[:, LANES:])
            level_band = lax.shift_right_logical(cell, (LANES - 1).bit_length())
            lat = group * 2 + jnp.where(first, 0, 1)
            lat = lat * lat_dev + lax.rem(level_band, lat_dev)
            lon = owner[b] * lon_dev + lax.div(level_band, lat_dev)
            row = (batches - 1 - turn) * 2 + side
            lon_at[pl.ds(row, 1), :] = lon.astype(F32)
            lat = lat.astype(F32) / lat_total
            lat_at[pl.ds(row, 1), :] = lat
            slope_at[pl.ds(row, 1), :] = lat * (-side_sign if side == 0 else side_sign)

    own_lon = (column * lon_dev + lane // lat_dev).astype(F32)
    own_lat = (band * lat_dev + lane % lat_dev).astype(F32) / lat_total

    def lon_factor(places, lon):
        gap = jnp.abs(places - lon)
        gap = jnp.minimum(gap, lon_total - gap)
        return jnp.maximum(0.0, 1.0 - gap / reach_span)

    def symmetric(buffer, slot):
        top = buffer[slot, : 2 * quarter, :]
        corner = buffer[slot, 2 * quarter :, 2 * quarter :]
        bottom = jnp.concatenate([top[:, 2 * quarter :].T, corner], axis=1)
        high, low = split(jnp.concatenate([top, bottom], axis=0))
        return high.astype(BF16), low.astype(BF16)

    def thrice(high, low, right_high, right_low):
        count = high.shape[0]
        both = dot(jnp.concatenate([high, low], axis=0).astype(BF16), right_high)
        return both[:count] + both[count:] + dot(high.astype(BF16), right_low)

    def prepare(turn, p, z):
        z_high, z_low = split(z[:members])
        pad = jnp.zeros((obs - 3 * members, obs), F32)
        zcat[p] = jnp.concatenate([z_high, z_high, z_low, pad], axis=0).T.astype(BF16)
        d_high, d_low = split(z[members:])
        slot = lax.rem(turn, SLOTS)
        v = thrice(z_high, z_low, *symmetric(root, slot))
        u = thrice(d_high, d_low, *symmetric(gain, slot))
        w = jnp.concatenate([v, u], axis=0) * (1.0 / (members - 1.0))
        w_high, w_low = split(w)
        fill = jnp.zeros((wcat.shape[1] // 2 - rows, obs), F32)
        wcat[p] = jnp.concatenate([w_high, fill, w_low, fill], axis=0).astype(BF16)

        base = (owner[order[turn]] * lon_dev).astype(F32)
        near[p] = lon_factor(lon_at[...], base)
        far[p] = lon_factor(lon_at[...], base + 1.0)
        for side in range(2):
            row = (batches - 1 - turn) * 2 + side
            lat_row = jnp.broadcast_to(lat_at[pl.ds(row, 1), :], (LANES, LANES))
            bit_row = jnp.broadcast_to(lon_at[pl.ds(row, 1), :] - base, (LANES, LANES))
            span = slice(side * LANES, (side + 1) * LANES)
            lat_column = lat_row.T
            lat_of[p, span, :] = lat_column
            rise_of[p, span, :] = 1.0 - lat_column * (side_sign if side == 0 else -side_sign)
            bit_of[p, span, :] = bit_row.T
        own_near = lon_factor(own_lon, base)
        own_far = lon_factor(own_lon, base + 1.0)
        lat_part = 1.0 - jnp.abs(lat_of[p] - own_lat)
        own_taper[p] = lat_part * jnp.where(bit_of[p] > 0.5, own_far, own_near)

    def covariance(p, start, width):
        now = state[:members, pl.ds(start, width)]
        high, low = split(now)
        zeros = jnp.zeros((obs - 3 * members, width), F32)
        right = jnp.concatenate([high, low, high, zeros], axis=0).astype(BF16)
        return dot(zcat[p], right)

    def updated(p, start, width, kind, row, cov):
        tiles = range(width // LANES)
        if kind == "obs":
            near_row = [near[p, pl.ds(row + k, 1), :] for k in tiles]
            far_row = [far[p, pl.ds(row + k, 1), :] for k in tiles]
            lat_row = [lat_at[pl.ds(row + k, 1), :] for k in tiles]
            slope_row = [slope_at[pl.ds(row + k, 1), :] for k in tiles]
        highs, lows = [], []
        for j in range(0, obs, STRIP):
            span = slice(j, j + STRIP)
            if kind == "obs":
                lat, rise = lat_of[p, span, :], rise_of[p, span, :]
                is_far = bit_of[p, span, :] > 0.5
            strip = []
            for k in tiles:
                if kind == "obs":
                    if (j < 2 * quarter) == (k % 2 == 0):
                        lat_part = 1.0 - jnp.abs(lat - lat_row[k])
                    else:
                        lat_part = rise + slope_row[k]
                    factor = lat_part * jnp.where(is_far, far_row[k], near_row[k])
                else:
                    factor = jnp.broadcast_to(
                        own_taper[p, span, row + k : row + k + 1], (STRIP, LANES)
                    )
                strip.append(cov[span, k * LANES : (k + 1) * LANES] * factor)
            strip = jnp.concatenate(strip, axis=1)
            high = strip.astype(BF16)
            highs.append(high)
            lows.append((strip - high.astype(F32)).astype(BF16))
        g_high = jnp.concatenate(highs, axis=0)
        g_low = jnp.concatenate(lows, axis=0)
        deep = wcat.shape[1] // 2
        both = dot(wcat[p], g_high)
        change = both[:deep] + both[deep:] + dot(wcat[p, :deep, :], g_low)
        return state[:, pl.ds(start, width)] - change[:rows]

    wide = CHUNK // LANES

    def assimilate(turn, p, later):
        coming = jnp.minimum(turn + 1, batches - 1)
        row = (batches - 1 - coming) * 2
        at = pl.multiple_of(own_cells + row * LANES, obs)
        work = [(at, obs, "obs", row)]
        for c in reversed(range(later)):
            work.append((own_cells + c * CHUNK, CHUNK, "obs", c * wide))
        for c in range(own_cells // CHUNK):
            work.append((c * CHUNK, CHUNK, "own", c * wide))
        ready = covariance(p, *work[0][:2])
        z = None
        for i, (start, width, kind, first_row) in enumerate(work):
            cov = ready
            if i + 1 < len(work):
                ready = covariance(p, *work[i + 1][:2])
            value = updated(p, start, width, kind, first_row, cov)
            if i == 0:
                z = value
            else:
                state[:, pl.ds(start, width)] = value
            if i == LAG:
                prepare(coming, 1 - p, z)

    for turn in range(1, SLOTS - 1):
        for copy in loads(turn, turn):
            copy.start()
    for copy in loads(0, 0):
        copy.wait()
    first_at = own_cells + (batches - 1) * obs
    prepare(jnp.int32(0), 0, state[:, first_at : first_at + obs])
    for group in range(0, batches, GROUP):
        later = max(0, -(-(batches - 2 - group) * obs // CHUNK))

        @pl.loop(group, group + GROUP, step=2)
        def _(turn, later=later):
            for copy in loads(turn + 1, lax.rem(turn + 1, SLOTS)):
                copy.wait()

            @pl.when(turn + 2 < batches)
            def _():
                for copy in loads(turn + 2, lax.rem(turn + 2, SLOTS)):
                    copy.wait()
                for copy in loads(turn + 3, lax.rem(turn + 3, SLOTS)):
                    copy.start()

            @pl.when(turn + 4 < batches)
            def _():
                for copy in loads(turn + 4, lax.rem(turn + 4, SLOTS)):
                    copy.start()

            assimilate(turn, 0, later)
            assimilate(turn + 1, 1, later)

    for k in range(own_tiles):
        span = slice(k * LANES, (k + 1) * LANES)
        anom_out[pl.ds(k, members, stride=own_tiles), :] = state[:members, span]
        mean_out[k : k + 1, :] = -state[members : members + 1, span]


def local(anomalies, state_mean, obs_value, obs_cell, owner, order, root_inv, gain_inv):
    members, lon_dev, lat_dev, levels = anomalies.shape
    batches, quarter = obs_value.shape
    obs = obs_cell.shape[1]
    blocks = lon_dev * lat_dev
    own_cells = blocks * levels
    slabs = lax.axis_size("gx")
    bands = lax.axis_size("gy")
    column = lax.axis_index("gx")
    band = lax.axis_index("gy")
    rows = -(-(members + 1) // 8) * 8
    tiles = batches * obs // LANES
    place = jnp.stack([column, band]).astype(jnp.int32)

    start = lax.div(band, 2) * 2 * quarter
    cut = functools.partial(
        lax.dynamic_slice_in_dim, start_index=start, slice_size=2 * quarter, axis=2
    )
    sent = [cut(root_inv), cut(gain_inv)]
    matrices = [
        [root_inv, swapped(root_inv, "gy", 1), swapped(sent[0], "gy", 2)],
        [gain_inv, swapped(gain_inv, "gy", 1), swapped(sent[1], "gy", 2)],
    ]
    for group in matrices:
        group.append(swapped(group[2], "gy", 1))

    smem = pl.BlockSpec(memory_space=pltpu.SMEM)
    vmem = pl.BlockSpec(memory_space=pltpu.VMEM)
    hbm = pl.BlockSpec(memory_space=pl.ANY)
    pairs = batches // 2
    piece = jax.ShapeDtypeStruct((rows, pairs // 2 * LANES), F32)
    own, keep, send = pl.pallas_call(
        functools.partial(gather_kernel, (members, blocks, quarter, pairs)),
        out_shape=(jax.ShapeDtypeStruct((rows, own_cells), F32), piece, piece),
        in_specs=[smem, smem, smem, vmem, vmem, vmem, vmem],
        out_specs=(vmem, vmem, vmem),
        scratch_shapes=[pltpu.VMEM((3 * rows, own_cells), BF16)],
        name="gather_observations",
    )(
        order,
        owner,
        place,
        obs_cell,
        anomalies.reshape(members * blocks, levels),
        state_mean.reshape(blocks, levels),
        jnp.concatenate([obs_value, obs_value], axis=1),
    )

    mine = keep + swapped(send, "gx", 1)
    mask = 2
    while mask < slabs:
        mine = mine + swapped(mine, "gx", mask)
        mask *= 2
    other = swapped(mine, "gx", 1)
    chip = [mine, other, swapped(mine, "gy", 2), swapped(other, "gy", 2)]
    pieces = chip + [swapped(part, "gy", 1) for part in chip]

    dims = (members, lon_dev, lat_dev, quarter, batches, slabs, bands)
    post, post_mean = pl.pallas_call(
        functools.partial(chain_kernel, dims),
        out_shape=(
            jax.ShapeDtypeStruct((members * blocks, levels), F32),
            jax.ShapeDtypeStruct((blocks, levels), F32),
        ),
        in_specs=[smem, smem, smem] + [vmem] * 10 + [hbm] * 8,
        out_specs=(vmem, vmem),
        scratch_shapes=[
            pltpu.VMEM((rows, own_cells + batches * obs), F32),
            pltpu.VMEM((tiles, LANES), F32),
            pltpu.VMEM((tiles, LANES), F32),
            pltpu.VMEM((tiles, LANES), F32),
            pltpu.VMEM((2, tiles, LANES), F32),
            pltpu.VMEM((2, tiles, LANES), F32),
            pltpu.VMEM((2, obs, obs), BF16),
            pltpu.VMEM((2, 2 * (-(-rows // 16) * 16), obs), BF16),
            pltpu.VMEM((2, obs, LANES), F32),
            pltpu.VMEM((2, obs, LANES), F32),
            pltpu.VMEM((2, obs, LANES), F32),
            pltpu.VMEM((2, obs, LANES), F32),
            pltpu.VMEM((SLOTS, obs, obs), F32),
            pltpu.VMEM((SLOTS, obs, obs), F32),
            pltpu.SemaphoreType.DMA((SLOTS, 12)),
        ],
        name="observation_recursion",
        compiler_params=pltpu.CompilerParams(

        ),
    )(order, owner, place, obs_cell, own, *pieces, *matrices[0], *matrices[1])
    return (
        post.reshape(members, lon_dev, lat_dev, levels),
        post_mean.reshape(lon_dev, lat_dev, levels),
    )


def solution(mesh):
    return jax.shard_map(
        local,
        mesh=mesh,
        in_specs=(
            P(None, "gx", "gy", None),
            P("gx", "gy", None),
            P(None, "gy"),
            P(),
            P(),
            P(),
            P(None, "gy", None),
            P(None, "gy", None),
        ),
        out_specs=(P(None, "gx", "gy", None), P("gx", "gy", None)),
        check_vma=False,
    )
```

```python
import functools
import jax
import jax.numpy as jnp
from jax import lax
from jax.experimental import pallas as pl
from jax.experimental.pallas import tpu as pltpu
from jax.sharding import PartitionSpec as P

REACH = 3
LANES = 128
CHUNK = 512
GROUP = 4
LAG = 2
DEPTH = 1
HOIST = 16
GATHER_BYTES = 12 * 2**20
CHAIN_BYTES = 20 * 2**20
STRIP = 16
F32 = jnp.float32
BF16 = jnp.bfloat16


def swapped(value, axis, mask):
    count = lax.axis_size(axis)
    return lax.ppermute(value, axis, [(source, source ^ mask) for source in range(count)])


def split(value):
    high = value.astype(BF16).astype(F32)
    return high, value - high


def dot(left, right):
    return jnp.dot(left, right, preferred_element_type=F32)


def gather_kernel(
    dims, order, owner, cells, anom, mean, obs, own_out, keep_out, send_out, parts
):
    members, blocks, quarter, pairs = dims
    rows = own_out.shape[0]
    column, band = lax.axis_index("gx"), lax.axis_index("gy")
    half = lax.rem(column, 2)
    for k in range(blocks):
        block = anom[pl.ds(k, members, stride=blocks), :]
        extra = jnp.concatenate(
            [-mean[k : k + 1, :], jnp.zeros((rows - members - 1, LANES), F32)], axis=0
        )
        block = jnp.concatenate([block, extra], axis=0)
        own_out[:, k * LANES : (k + 1) * LANES] = block
        high, rest = split(block)
        mid, low = split(rest)
        stack = jnp.concatenate([high, mid, low], axis=0)
        parts[:, k * LANES : (k + 1) * LANES] = stack.astype(BF16)
    lane = lax.broadcasted_iota(jnp.int32, (1, LANES), 1)
    first = lane < quarter
    total = cells.shape[1]
    shift = lax.rem(total - band * quarter, total)

    def ids_of(pair):
        even, odd = order[2 * pair], order[2 * pair + 1]
        row_even = pltpu.roll(cells[pl.ds(even, 1), :], shift, 1)[:, :LANES]
        row_odd = pltpu.roll(cells[pl.ds(odd, 1), :], lax.rem(shift + quarter, total), 1)
        row_odd = row_odd[:, :LANES]
        here_even = owner[even] == column
        here_odd = owner[odd] == column
        mine = jnp.where(first, here_even.astype(jnp.int32), here_odd.astype(jnp.int32))
        ids = jnp.where(mine > 0, jnp.where(first, row_even, row_odd), -1)
        seen = jnp.concatenate([obs[pl.ds(even, 1), :], obs[pl.ds(odd, 1), :]], axis=1)
        seen = jnp.where(mine > 0, seen, 0.0)
        return ids, seen, jnp.logical_or(here_even, here_odd)

    for out, which in ((keep_out, half), (send_out, 1 - half)):
        for slot in range(0, pairs // 2, 2):
            pair = which * (pairs // 2) + slot
            ids_a, seen_a, any_a = ids_of(pair)
            ids_b, seen_b, any_b = ids_of(pair + 1)
            ids = jnp.concatenate([ids_a, ids_b], axis=1)
            seen = jnp.concatenate([seen_a, seen_b], axis=1)
            span = slice(slot * LANES, (slot + 2) * LANES)
            busy = jnp.logical_or(any_a, any_b)

            @pl.when(busy)
            def _(out=out, ids=ids, seen=seen, span=span):
                total_cells = parts.shape[1]
                cell = lax.broadcasted_iota(jnp.int32, (total_cells, 2 * LANES), 0)
                hot = jnp.where(cell == ids, 1.0, 0.0).astype(BF16)
                found = dot(parts[...], hot)
                value = found[:rows] + found[rows : 2 * rows] + found[2 * rows :]
                row = lax.broadcasted_iota(jnp.int32, value.shape, 0)
                out[:, span] = value + jnp.where(row == members, seen, 0.0)

            @pl.when(jnp.logical_not(busy))
            def _(out=out, span=span):
                out[:, span] = jnp.zeros((rows, 2 * LANES), F32)


def pack_kernel(root, gain, out):
    batches, quarter = root.shape[:2]
    band = lax.axis_index("gy")
    core, chip = lax.rem(band, 2), lax.div(band, 2)
    near = pl.ds(pl.multiple_of(chip * LANES, LANES), LANES)
    first = lax.broadcasted_iota(jnp.int32, (1, LANES), 1) < quarter
    stride = batches // 2 + batches // 4
    for kind, source in enumerate((root, gain)):

        def joined(left, right, own_half_is_left):
            left = jnp.where(own_half_is_left, left, pltpu.roll(left, quarter, 1))
            right = jnp.where(own_half_is_left, pltpu.roll(right, quarter, 1), right)
            return jnp.where(first, left, right)

        for k in range(batches // 2):
            out[kind * stride + k] = joined(
                source[2 * k, :, near], source[2 * k + 1, :, near], core == 0
            )
        for k in range(batches // 4):
            out[kind * stride + batches // 2 + k] = joined(
                source[4 * k + core, :, near], source[4 * k + 2 + core, :, near], core != 0
            )


def chain_kernel(
    dims,
    order,
    owner,
    cells,
    own,
    *refs,
):
    members, lon_dev, lat_dev, quarter, batches, slabs, bands = dims
    pieces = refs[:8]
    locals_, partners, across, relayed = refs[8:10], refs[10:12], refs[12], refs[13]
    anom_out, mean_out = refs[14:16]
    state, own_state, lon_at, lat_at, slope_at, near, far, zcat, wcat = refs[16:25]
    lat_of, rise_of, bit_of, own_taper = refs[25:]
    rows = state.shape[0]
    own_cells = own.shape[1]
    own_tiles = own_cells // LANES
    obs = bands * quarter
    column, band = lax.axis_index("gx"), lax.axis_index("gy")
    core = lax.rem(band, 2)
    chip = lax.div(band, 2)
    lat_total = float(bands * lat_dev)
    lon_total = float(slabs * lon_dev)
    reach_span = REACH * lon_dev + 1.0

    own_state[...] = own[...]
    lane = lax.broadcasted_iota(jnp.int32, (1, LANES), 1)
    first = lane < quarter
    low_core = jnp.where(first, 1, 0) * jnp.where(core == 0, 1, 0) + jnp.where(
        first, 0, 1
    ) * jnp.where(core == 0, 0, 1)
    from_self = low_core > 0
    half_pairs = batches // 4
    half = lax.rem(column, 2)
    for which in range(2):
        pair_base = (half if which == 0 else 1 - half) * half_pairs
        for side in range(2):
            mine = pieces[2 * side + which]
            theirs = pieces[4 + 2 * side + which]
            for k in range(half_pairs):
                span = slice(k * LANES, (k + 1) * LANES)
                a, b = mine[:, span], theirs[:, span]
                a_roll, b_roll = pltpu.roll(a, quarter, 1), pltpu.roll(b, quarter, 1)
                a_first, b_first = (
                    jnp.where(core == 0, a, a_roll),
                    jnp.where(core == 0, b_roll, b),
                )
                a_last, b_last = (
                    jnp.where(core == 0, a_roll, a),
                    jnp.where(core == 0, b, b_roll),
                )
                turn = 2 * (pair_base + k)
                for step, (x, y) in enumerate(((a_first, b_first), (a_last, b_last))):
                    at = (batches - 1 - turn - step) * obs + side * LANES
                    at = pl.multiple_of(at, LANES)
                    state[:, pl.ds(at, LANES)] = jnp.where(from_self, x, y)

    side_sign = jnp.where(chip > 0, 1.0, -1.0)

    @pl.loop(0, batches)
    def _(turn):
        b = order[turn]
        cells_row = cells[pl.ds(b, 1), :]
        for side in range(2):
            group = chip if side == 0 else 1 - chip
            cell = jnp.where(group == 0, cells_row[:, :LANES], cells_row[:, LANES:])
            level_band = lax.shift_right_logical(cell, (LANES - 1).bit_length())
            lat = group * 2 + jnp.where(first, 0, 1)
            lat = lat * lat_dev + lax.rem(level_band, lat_dev)
            lon = owner[b] * lon_dev + lax.div(level_band, lat_dev)
            row = (batches - 1 - turn) * 2 + side
            lon_at[pl.ds(row, 1), :] = lon.astype(F32)
            lat = lat.astype(F32) / lat_total
            lat_at[pl.ds(row, 1), :] = lat
            slope_at[pl.ds(row, 1), :] = lat * (-side_sign if side == 0 else side_sign)

    own_lon = (column * lon_dev + lane // lat_dev).astype(F32)
    own_lat = (band * lat_dev + lane % lat_dev).astype(F32) / lat_total

    def lon_factor(places, lon):
        gap = jnp.abs(places - lon)
        gap = jnp.minimum(gap, lon_total - gap)
        return jnp.maximum(0.0, 1.0 - gap / reach_span)

    near_cols = pl.ds(pl.multiple_of(chip * LANES, LANES), LANES)
    far_cols = pl.ds(pl.multiple_of((1 - chip) * LANES, LANES), LANES)
    stride = batches // 2 + batches // 4

    def by_core(mine, theirs):
        is_even = core == 0
        return jnp.where(is_even, mine, theirs), jnp.where(is_even, theirs, mine)

    def symmetric(kind, b):
        mine, theirs = locals_[kind], partners[kind]
        blocks = [
            jnp.concatenate(by_core(mine[b, :, cols], theirs[b, :, cols]), axis=0)
            for cols in (near_cols, far_cols)
        ]
        pair, odd = lax.div(b, 2), lax.rem(b, 2)
        at = kind * stride + pair
        even_tile, odd_tile = by_core(across[at], relayed[at])
        even_even = jnp.where(odd == 0, even_tile, pltpu.roll(even_tile, quarter, 1))
        odd_odd = jnp.where(odd == 0, pltpu.roll(odd_tile, quarter, 1), odd_tile)
        at = kind * stride + batches // 2 + lax.div(pair, 2)
        cross = jnp.where(odd == core, across[at], relayed[at])
        turned = pltpu.roll(cross, quarter, 1)
        is_left = lax.rem(pair, 2) == 0
        cross, turned = jnp.where(is_left, cross, turned), jnp.where(is_left, turned, cross)
        cross = jnp.where(first, cross, turned)
        flipped = jnp.concatenate([cross, cross], axis=0).T[:quarter]
        even_odd = jnp.where(odd == 0, cross, flipped)
        odd_even = jnp.where(odd == 0, flipped, cross)
        corner = jnp.concatenate(
            [jnp.where(first, even_even, even_odd), jnp.where(first, odd_even, odd_odd)], axis=0
        )
        whole = jnp.concatenate(
            [
                jnp.concatenate(blocks, axis=1),
                jnp.concatenate([blocks[1].T, corner], axis=1),
            ],
            axis=0,
        )
        high, low = split(whole)
        return high.astype(BF16), low.astype(BF16)

    def thrice(high, low, right_high, right_low):
        count = high.shape[0]
        both = dot(jnp.concatenate([high, low], axis=0).astype(BF16), right_high)
        return both[:count] + both[count:] + dot(high.astype(BF16), right_low)

    def prepare(turn, p, z):
        z_high, z_low = split(z[:members])
        pad = jnp.zeros((obs - 3 * members, obs), F32)
        zcat[p] = jnp.concatenate([z_high, z_high, z_low, pad], axis=0).T.astype(BF16)
        d_high, d_low = split(z[members:])
        v = thrice(z_high, z_low, *symmetric(0, order[turn]))
        u = thrice(d_high, d_low, *symmetric(1, order[turn]))
        w = jnp.concatenate([v, u], axis=0) * (1.0 / (members - 1.0))
        w_high, w_low = split(w)
        fill = jnp.zeros((wcat.shape[1] // 2 - rows, obs), F32)
        wcat[p] = jnp.concatenate([w_high, fill, w_low, fill], axis=0).astype(BF16)

        base = (owner[order[turn]] * lon_dev).astype(F32)
        near[p] = lon_factor(lon_at[...], base)
        far[p] = lon_factor(lon_at[...], base + 1.0)
        for side in range(2):
            row = (batches - 1 - turn) * 2 + side
            lat_row = jnp.broadcast_to(lat_at[pl.ds(row, 1), :], (LANES, LANES))
            bit_row = jnp.broadcast_to(lon_at[pl.ds(row, 1), :] - base, (LANES, LANES))
            span = slice(side * LANES, (side + 1) * LANES)
            lat_column = lat_row.T
            lat_of[p, span, :] = lat_column
            rise_of[p, span, :] = 1.0 - lat_column * (side_sign if side == 0 else -side_sign)
            bit_of[p, span, :] = bit_row.T
        own_near = lon_factor(own_lon, base)
        own_far = lon_factor(own_lon, base + 1.0)
        lat_part = 1.0 - jnp.abs(lat_of[p] - own_lat)
        own_taper[p] = lat_part * jnp.where(bit_of[p] > 0.5, own_far, own_near)

    def covariance(p, start, width, kind, row):
        source = state if kind == "obs" else own_state
        now = source[:members, pl.ds(start, width)]
        high, low = split(now)
        zeros = jnp.zeros((obs - 3 * members, width), F32)
        right = jnp.concatenate([high, low, high, zeros], axis=0).astype(BF16)
        return dot(zcat[p], right)

    def updated(p, start, width, kind, row, cov):
        tiles = range(width // LANES)
        if kind == "obs":
            near_row = [near[p, pl.ds(row + k, 1), :] for k in tiles]
            far_row = [far[p, pl.ds(row + k, 1), :] for k in tiles]
            lat_row = [lat_at[pl.ds(row + k, 1), :] for k in tiles]
            slope_row = [slope_at[pl.ds(row + k, 1), :] for k in tiles]
        highs, lows = [], []
        for j in range(0, obs, STRIP):
            span = slice(j, j + STRIP)
            if kind == "obs":
                lat, rise = lat_of[p, span, :], rise_of[p, span, :]
                is_far = bit_of[p, span, :] > 0.5
            strip = []
            for k in tiles:
                if kind == "obs":
                    if (j < 2 * quarter) == (k % 2 == 0):
                        lat_part = 1.0 - jnp.abs(lat - lat_row[k])
                    else:
                        lat_part = rise + slope_row[k]
                    factor = lat_part * jnp.where(is_far, far_row[k], near_row[k])
                else:
                    factor = jnp.broadcast_to(
                        own_taper[p, span, row + k : row + k + 1], (STRIP, LANES)
                    )
                strip.append(cov[span, k * LANES : (k + 1) * LANES] * factor)
            strip = jnp.concatenate(strip, axis=1)
            high = strip.astype(BF16)
            highs.append(high)
            lows.append((strip - high.astype(F32)).astype(BF16))
        g_high = jnp.concatenate(highs, axis=0)
        g_low = jnp.concatenate(lows, axis=0)
        deep = wcat.shape[1] // 2
        both = dot(wcat[p], g_high)
        change = both[:deep] + both[deep:] + dot(wcat[p, :deep, :], g_low)
        source = state if kind == "obs" else own_state
        return source[:, pl.ds(start, width)] - change[:rows]

    wide = CHUNK // LANES

    def assimilate(turn, p, later):
        coming = jnp.minimum(turn + 1, batches - 1)
        row = (batches - 1 - coming) * 2
        at = pl.multiple_of(row * LANES, obs)
        work = [(at, obs, "obs", row)]
        for c in reversed(range(later)):
            work.append((c * CHUNK, CHUNK, "obs", c * wide))
        for c in range(own_cells // CHUNK):
            work.append((c * CHUNK, CHUNK, "own", c * wide))
        ready = [covariance(p, *item) for item in work[:DEPTH]]
        z = None
        for i, item in enumerate(work):
            if i + DEPTH < len(work):
                ready.append(covariance(p, *work[i + DEPTH]))
            value = updated(p, *item, ready[i])
            if i == 0:
                z = value
            else:
                target = state if item[2] == "obs" else own_state
                target[:, pl.ds(item[0], item[1])] = value
            if i == LAG:
                prepare(coming, 1 - p, z)

    first_at = (batches - 1) * obs
    prepare(jnp.int32(0), 0, state[:, first_at : first_at + obs])
    for group in range(0, batches, GROUP):
        later = max(0, -(-(batches - 2 - group) * obs // CHUNK))

        @pl.loop(group, group + GROUP, step=2)
        def _(turn, later=later):
            assimilate(turn, 0, later)
            assimilate(turn + 1, 1, later)

    for k in range(own_tiles):
        span = slice(k * LANES, (k + 1) * LANES)
        anom_out[pl.ds(k, members, stride=own_tiles), :] = own_state[:members, span]
        mean_out[k : k + 1, :] = -own_state[members : members + 1, span]


def local(anomalies, state_mean, obs_value, obs_cell, owner, order, root_inv, gain_inv):
    members, lon_dev, lat_dev, levels = anomalies.shape
    batches, quarter = obs_value.shape
    obs = obs_cell.shape[1]
    blocks = lon_dev * lat_dev
    own_cells = blocks * levels
    slabs = lax.axis_size("gx")
    bands = lax.axis_size("gy")
    rows = -(-(members + 1) // 8) * 8
    tiles = batches * obs // LANES

    smem = pl.BlockSpec(memory_space=pltpu.SMEM)
    vmem = pl.BlockSpec(memory_space=pltpu.VMEM)
    pairs = batches // 2
    piece = jax.ShapeDtypeStruct((rows, pairs // 2 * LANES), F32)
    own, keep, send = pl.pallas_call(
        functools.partial(gather_kernel, (members, blocks, quarter, pairs)),
        out_shape=(jax.ShapeDtypeStruct((rows, own_cells), F32), piece, piece),
        in_specs=[smem, smem, vmem, vmem, vmem, vmem],
        out_specs=(vmem, vmem, vmem),
        scratch_shapes=[pltpu.VMEM((3 * rows, own_cells), BF16)],
        name="gather_observations",
        compiler_params=pltpu.CompilerParams(vmem_limit_bytes=GATHER_BYTES),
    )(
        order,
        owner,
        obs_cell,
        anomalies.reshape(members * blocks, levels),
        state_mean.reshape(blocks, levels),
        obs_value,
    )

    packed = pl.pallas_call(
        pack_kernel,
        out_shape=jax.ShapeDtypeStruct(
            (2 * (batches // 2 + batches // 4), quarter, LANES), F32
        ),
        in_specs=[vmem, vmem],
        out_specs=vmem,
        name="pack_matrices",
        compiler_params=pltpu.CompilerParams(vmem_limit_bytes=GATHER_BYTES),
    )(root_inv, gain_inv)
    across = swapped(packed, "gy", 2)
    partners = [swapped(root_inv, "gy", 1), swapped(gain_inv, "gy", 1)]

    mine = keep + swapped(send, "gx", 1)
    mask = 2
    while mask < slabs:
        mine = mine + swapped(mine, "gx", mask)
        mask *= 2
    other = swapped(mine, "gx", 1)
    chip = [mine, other, swapped(mine, "gy", 2), swapped(other, "gy", 2)]
    pieces = chip + [swapped(part, "gy", 1) for part in chip]

    dims = (members, lon_dev, lat_dev, quarter, batches, slabs, bands)
    post, post_mean = pl.pallas_call(
        functools.partial(chain_kernel, dims),
        out_shape=(
            jax.ShapeDtypeStruct((members * blocks, levels), F32),
            jax.ShapeDtypeStruct((blocks, levels), F32),
        ),
        in_specs=[smem, smem] + [vmem] * 16,
        out_specs=(vmem, vmem),
        scratch_shapes=[
            pltpu.VMEM((rows, batches * obs), F32),
            pltpu.VMEM((rows, own_cells), F32),
            pltpu.VMEM((tiles, LANES), F32),
            pltpu.VMEM((tiles, LANES), F32),
            pltpu.VMEM((tiles, LANES), F32),
            pltpu.VMEM((2, tiles, LANES), F32),
            pltpu.VMEM((2, tiles, LANES), F32),
            pltpu.VMEM((2, obs, obs), BF16),
            pltpu.VMEM((2, 2 * (-(-rows // 16) * 16), obs), BF16),
            pltpu.VMEM((2, obs, LANES), F32),
            pltpu.VMEM((2, obs, LANES), F32),
            pltpu.VMEM((2, obs, LANES), F32),
            pltpu.VMEM((2, obs, LANES), F32),
        ],
        name="observation_recursion",
        compiler_params=pltpu.CompilerParams(
            vmem_limit_bytes=CHAIN_BYTES
        ),
    )(
        order,
        owner,
        obs_cell,
        own,
        *pieces,
        root_inv,
        gain_inv,
        *partners,
        across,
        swapped(across, "gy", 1),
    )
    return (
        post.reshape(members, lon_dev, lat_dev, levels),
        post_mean.reshape(lon_dev, lat_dev, levels),
    )


def solution(mesh):
    return jax.shard_map(
        local,
        mesh=mesh,
        in_specs=(
            P(None, "gx", "gy", None),
            P("gx", "gy", None),
            P(None, "gy"),
            P(),
            P(),
            P(),
            P(None, "gy", None),
            P(None, "gy", None),
        ),
        out_specs=(P(None, "gx", "gy", None), P("gx", "gy", None)),
        check_vma=False,
    )
```

```python
import functools
import jax
import jax.numpy as jnp
from jax import lax
from jax.experimental import pallas as pl
from jax.experimental.pallas import tpu as pltpu
from jax.sharding import PartitionSpec as P

REACH = 3
LANES = 128
CHUNK = 512
GROUP = 4
LAG = 2
LATE_LAG = 4
LOOPED = 4
DEPTH = 1
HOIST = 16
GATHER_BYTES = 12 * 2**20
CHAIN_BYTES = 20 * 2**20
STRIP = 16
F32 = jnp.float32
BF16 = jnp.bfloat16


def swapped(value, axis, mask):
    count = lax.axis_size(axis)
    return lax.ppermute(value, axis, [(source, source ^ mask) for source in range(count)])


def split(value):
    high = value.astype(BF16).astype(F32)
    return high, value - high


def dot(left, right):
    return jnp.dot(left, right, preferred_element_type=F32)


def gather_kernel(
    dims, order, owner, cells, anom, mean, obs, own_out, keep_out, send_out, parts
):
    members, blocks, quarter, pairs = dims
    rows = own_out.shape[0]
    column, band = lax.axis_index("gx"), lax.axis_index("gy")
    half = lax.rem(column, 2)
    for k in range(blocks):
        block = anom[pl.ds(k, members, stride=blocks), :]
        extra = jnp.concatenate(
            [-mean[k : k + 1, :], jnp.zeros((rows - members - 1, LANES), F32)], axis=0
        )
        block = jnp.concatenate([block, extra], axis=0)
        own_out[:, k * LANES : (k + 1) * LANES] = block
        high, rest = split(block)
        mid, low = split(rest)
        stack = jnp.concatenate([high, mid, low], axis=0)
        parts[:, k * LANES : (k + 1) * LANES] = stack.astype(BF16)
    lane = lax.broadcasted_iota(jnp.int32, (1, LANES), 1)
    first = lane < quarter
    total = cells.shape[1]
    shift = lax.rem(total - band * quarter, total)

    def ids_of(pair):
        even, odd = order[2 * pair], order[2 * pair + 1]
        row_even = pltpu.roll(cells[pl.ds(even, 1), :], shift, 1)[:, :LANES]
        row_odd = pltpu.roll(cells[pl.ds(odd, 1), :], lax.rem(shift + quarter, total), 1)
        row_odd = row_odd[:, :LANES]
        here_even = owner[even] == column
        here_odd = owner[odd] == column
        mine = jnp.where(first, here_even.astype(jnp.int32), here_odd.astype(jnp.int32))
        ids = jnp.where(mine > 0, jnp.where(first, row_even, row_odd), -1)
        seen = jnp.concatenate([obs[pl.ds(even, 1), :], obs[pl.ds(odd, 1), :]], axis=1)
        seen = jnp.where(mine > 0, seen, 0.0)
        return ids, seen, jnp.logical_or(here_even, here_odd)

    for out, which in ((keep_out, half), (send_out, 1 - half)):
        for slot in range(0, pairs // 2, 2):
            pair = which * (pairs // 2) + slot
            ids_a, seen_a, any_a = ids_of(pair)
            ids_b, seen_b, any_b = ids_of(pair + 1)
            ids = jnp.concatenate([ids_a, ids_b], axis=1)
            seen = jnp.concatenate([seen_a, seen_b], axis=1)
            span = slice(slot * LANES, (slot + 2) * LANES)
            busy = jnp.logical_or(any_a, any_b)

            @pl.when(busy)
            def _(out=out, ids=ids, seen=seen, span=span):
                total_cells = parts.shape[1]
                cell = lax.broadcasted_iota(jnp.int32, (total_cells, 2 * LANES), 0)
                hot = jnp.where(cell == ids, 1.0, 0.0).astype(BF16)
                found = dot(parts[...], hot)
                value = found[:rows] + found[rows : 2 * rows] + found[2 * rows :]
                row = lax.broadcasted_iota(jnp.int32, value.shape, 0)
                out[:, span] = value + jnp.where(row == members, seen, 0.0)

            @pl.when(jnp.logical_not(busy))
            def _(out=out, span=span):
                out[:, span] = jnp.zeros((rows, 2 * LANES), F32)


def pack_kernel(root, gain, out):
    batches, quarter = root.shape[:2]
    band = lax.axis_index("gy")
    core, chip = lax.rem(band, 2), lax.div(band, 2)
    near = pl.ds(pl.multiple_of(chip * LANES, LANES), LANES)
    first = lax.broadcasted_iota(jnp.int32, (1, LANES), 1) < quarter
    stride = batches // 2 + batches // 4
    for kind, source in enumerate((root, gain)):

        def joined(left, right, own_half_is_left):
            left = jnp.where(own_half_is_left, left, pltpu.roll(left, quarter, 1))
            right = jnp.where(own_half_is_left, pltpu.roll(right, quarter, 1), right)
            return jnp.where(first, left, right)

        for k in range(batches // 2):
            out[kind * stride + k] = joined(
                source[2 * k, :, near], source[2 * k + 1, :, near], core == 0
            )
        for k in range(batches // 4):
            out[kind * stride + batches // 2 + k] = joined(
                source[4 * k + core, :, near], source[4 * k + 2 + core, :, near], core != 0
            )


def chain_kernel(
    dims,
    order,
    owner,
    cells,
    own,
    *refs,
):
    members, lon_dev, lat_dev, quarter, batches, slabs, bands = dims
    pieces = refs[:8]
    locals_, partners, across, relayed = refs[8:10], refs[10:12], refs[12], refs[13]
    anom_out, mean_out = refs[14:16]
    state, own_state, lon_at, lat_at, slope_at, near, far, zcat, wcat = refs[16:25]
    lat_of, rise_of, bit_of, own_taper = refs[25:]
    rows = state.shape[0]
    own_cells = own.shape[1]
    own_tiles = own_cells // LANES
    obs = bands * quarter
    column, band = lax.axis_index("gx"), lax.axis_index("gy")
    core = lax.rem(band, 2)
    chip = lax.div(band, 2)
    lat_total = float(bands * lat_dev)
    lon_total = float(slabs * lon_dev)
    reach_span = REACH * lon_dev + 1.0

    own_state[...] = own[...]
    lane = lax.broadcasted_iota(jnp.int32, (1, LANES), 1)
    first = lane < quarter
    low_core = jnp.where(first, 1, 0) * jnp.where(core == 0, 1, 0) + jnp.where(
        first, 0, 1
    ) * jnp.where(core == 0, 0, 1)
    from_self = low_core > 0
    half_pairs = batches // 4
    half = lax.rem(column, 2)
    for which in range(2):
        pair_base = (half if which == 0 else 1 - half) * half_pairs
        for side in range(2):
            mine = pieces[2 * side + which]
            theirs = pieces[4 + 2 * side + which]
            for k in range(half_pairs):
                span = slice(k * LANES, (k + 1) * LANES)
                a, b = mine[:, span], theirs[:, span]
                a_roll, b_roll = pltpu.roll(a, quarter, 1), pltpu.roll(b, quarter, 1)
                a_first, b_first = (
                    jnp.where(core == 0, a, a_roll),
                    jnp.where(core == 0, b_roll, b),
                )
                a_last, b_last = (
                    jnp.where(core == 0, a_roll, a),
                    jnp.where(core == 0, b, b_roll),
                )
                turn = 2 * (pair_base + k)
                for step, (x, y) in enumerate(((a_first, b_first), (a_last, b_last))):
                    at = (batches - 1 - turn - step) * obs + side * LANES
                    at = pl.multiple_of(at, LANES)
                    state[:, pl.ds(at, LANES)] = jnp.where(from_self, x, y)

    side_sign = jnp.where(chip > 0, 1.0, -1.0)

    @pl.loop(0, batches)
    def _(turn):
        b = order[turn]
        cells_row = cells[pl.ds(b, 1), :]
        for side in range(2):
            group = chip if side == 0 else 1 - chip
            cell = jnp.where(group == 0, cells_row[:, :LANES], cells_row[:, LANES:])
            level_band = lax.shift_right_logical(cell, (LANES - 1).bit_length())
            lat = group * 2 + jnp.where(first, 0, 1)
            lat = lat * lat_dev + lax.rem(level_band, lat_dev)
            lon = owner[b] * lon_dev + lax.div(level_band, lat_dev)
            row = (batches - 1 - turn) * 2 + side
            lon_at[pl.ds(row, 1), :] = lon.astype(F32)
            lat = lat.astype(F32) / lat_total
            lat_at[pl.ds(row, 1), :] = lat
            slope_at[pl.ds(row, 1), :] = lat * (-side_sign if side == 0 else side_sign)

    own_lon = (column * lon_dev + lane // lat_dev).astype(F32)
    own_lat = (band * lat_dev + lane % lat_dev).astype(F32) / lat_total

    def lon_factor(places, lon):
        gap = jnp.abs(places - lon)
        gap = jnp.minimum(gap, lon_total - gap)
        return jnp.maximum(0.0, 1.0 - gap / reach_span)

    near_cols = pl.ds(pl.multiple_of(chip * LANES, LANES), LANES)
    far_cols = pl.ds(pl.multiple_of((1 - chip) * LANES, LANES), LANES)
    stride = batches // 2 + batches // 4

    def by_core(mine, theirs):
        is_even = core == 0
        return jnp.where(is_even, mine, theirs), jnp.where(is_even, theirs, mine)

    def symmetric(kind, b):
        mine, theirs = locals_[kind], partners[kind]
        blocks = [
            jnp.concatenate(by_core(mine[b, :, cols], theirs[b, :, cols]), axis=0)
            for cols in (near_cols, far_cols)
        ]
        pair, odd = lax.div(b, 2), lax.rem(b, 2)
        at = kind * stride + pair
        even_tile, odd_tile = by_core(across[at], relayed[at])
        even_even = jnp.where(odd == 0, even_tile, pltpu.roll(even_tile, quarter, 1))
        odd_odd = jnp.where(odd == 0, pltpu.roll(odd_tile, quarter, 1), odd_tile)
        at = kind * stride + batches // 2 + lax.div(pair, 2)
        cross = jnp.where(odd == core, across[at], relayed[at])
        turned = pltpu.roll(cross, quarter, 1)
        is_left = lax.rem(pair, 2) == 0
        cross, turned = jnp.where(is_left, cross, turned), jnp.where(is_left, turned, cross)
        cross = jnp.where(first, cross, turned)
        flipped = jnp.concatenate([cross, cross], axis=0).T[:quarter]
        even_odd = jnp.where(odd == 0, cross, flipped)
        odd_even = jnp.where(odd == 0, flipped, cross)
        corner = jnp.concatenate(
            [jnp.where(first, even_even, even_odd), jnp.where(first, odd_even, odd_odd)], axis=0
        )
        whole = jnp.concatenate(
            [
                jnp.concatenate(blocks, axis=1),
                jnp.concatenate([blocks[1].T, corner], axis=1),
            ],
            axis=0,
        )
        high, low = split(whole)
        return high.astype(BF16), low.astype(BF16)

    def thrice(high, low, right_high, right_low):
        count = high.shape[0]
        both = dot(jnp.concatenate([high, low], axis=0).astype(BF16), right_high)
        return both[:count] + both[count:] + dot(high.astype(BF16), right_low)

    def prepare(turn, p, z):
        z_high, z_low = split(z[:members])
        pad = jnp.zeros((obs - 3 * members, obs), F32)
        zcat[p] = jnp.concatenate([z_high, z_high, z_low, pad], axis=0).T.astype(BF16)
        d_high, d_low = split(z[members:])
        v = thrice(z_high, z_low, *symmetric(0, order[turn]))
        u = thrice(d_high, d_low, *symmetric(1, order[turn]))
        w = jnp.concatenate([v, u], axis=0) * (1.0 / (members - 1.0))
        w_high, w_low = split(w)
        fill = jnp.zeros((wcat.shape[1] // 2 - rows, obs), F32)
        wcat[p] = jnp.concatenate([w_high, fill, w_low, fill], axis=0).astype(BF16)

        base = (owner[order[turn]] * lon_dev).astype(F32)
        near[p] = lon_factor(lon_at[...], base)
        far[p] = lon_factor(lon_at[...], base + 1.0)
        for side in range(2):
            row = (batches - 1 - turn) * 2 + side
            lat_row = jnp.broadcast_to(lat_at[pl.ds(row, 1), :], (LANES, LANES))
            bit_row = jnp.broadcast_to(lon_at[pl.ds(row, 1), :] - base, (LANES, LANES))
            span = slice(side * LANES, (side + 1) * LANES)
            lat_column = lat_row.T
            lat_of[p, span, :] = lat_column
            rise_of[p, span, :] = 1.0 - lat_column * (side_sign if side == 0 else -side_sign)
            bit_of[p, span, :] = bit_row.T
        own_near = lon_factor(own_lon, base)
        own_far = lon_factor(own_lon, base + 1.0)
        lat_part = 1.0 - jnp.abs(lat_of[p] - own_lat)
        own_taper[p] = lat_part * jnp.where(bit_of[p] > 0.5, own_far, own_near)

    def covariance(p, start, width, kind, row):
        source = state if kind == "obs" else own_state
        now = source[:members, pl.ds(start, width)]
        high, low = split(now)
        zeros = jnp.zeros((obs - 3 * members, width), F32)
        right = jnp.concatenate([high, low, high, zeros], axis=0).astype(BF16)
        return dot(zcat[p], right)

    def updated(p, start, width, kind, row, cov):
        tiles = range(width // LANES)
        if kind == "obs":
            near_row = [near[p, pl.ds(row + k, 1), :] for k in tiles]
            far_row = [far[p, pl.ds(row + k, 1), :] for k in tiles]
            lat_row = [lat_at[pl.ds(row + k, 1), :] for k in tiles]
            slope_row = [slope_at[pl.ds(row + k, 1), :] for k in tiles]
        highs, lows = [], []
        for j in range(0, obs, STRIP):
            span = slice(j, j + STRIP)
            if kind == "obs":
                lat, rise = lat_of[p, span, :], rise_of[p, span, :]
                is_far = bit_of[p, span, :] > 0.5
            strip = []
            for k in tiles:
                if kind == "obs":
                    if (j < 2 * quarter) == (k % 2 == 0):
                        lat_part = 1.0 - jnp.abs(lat - lat_row[k])
                    else:
                        lat_part = rise + slope_row[k]
                    factor = lat_part * jnp.where(is_far, far_row[k], near_row[k])
                else:
                    factor = jnp.broadcast_to(
                        own_taper[p, span, row + k : row + k + 1], (STRIP, LANES)
                    )
                strip.append(cov[span, k * LANES : (k + 1) * LANES] * factor)
            strip = jnp.concatenate(strip, axis=1)
            high = strip.astype(BF16)
            highs.append(high)
            lows.append((strip - high.astype(F32)).astype(BF16))
        g_high = jnp.concatenate(highs, axis=0)
        g_low = jnp.concatenate(lows, axis=0)
        deep = wcat.shape[1] // 2
        both = dot(wcat[p], g_high)
        change = both[:deep] + both[deep:] + dot(wcat[p, :deep, :], g_low)
        source = state if kind == "obs" else own_state
        return source[:, pl.ds(start, width)] - change[:rows]

    wide = CHUNK // LANES

    def assimilate(turn, p, later):
        work = []
        last = isinstance(turn, int) and turn + 1 == batches
        if not last:
            coming = turn + 1
            row = (batches - 1 - coming) * 2
            at = row * LANES if isinstance(row, int) else pl.multiple_of(row * LANES, obs)
            work.append((at, obs, "obs", row))
        for c in reversed(range(later)):
            work.append((c * CHUNK, CHUNK, "obs", c * wide))
        for c in range(own_cells // CHUNK):
            work.append((c * CHUNK, CHUNK, "own", c * wide))
        ready = [covariance(p, *item) for item in work[:DEPTH]]
        z = None
        for i, item in enumerate(work):
            if i + DEPTH < len(work):
                ready.append(covariance(p, *work[i + DEPTH]))
            value = updated(p, *item, ready[i])
            if i == 0 and not last:
                z = value
            else:
                target = state if item[2] == "obs" else own_state
                target[:, pl.ds(item[0], item[1])] = value
            if i == (LAG if later > 4 else LATE_LAG) and not last:
                prepare(coming, 1 - p, z)

    first_at = (batches - 1) * obs
    prepare(jnp.int32(0), 0, state[:, first_at : first_at + obs])
    for group in range(0, batches, GROUP):
        if group >= LOOPED:
            for turn in range(group, group + GROUP):
                assimilate(turn, turn % 2, max(0, -(-(batches - 2 - turn) * obs // CHUNK)))
            continue
        later = -(-(batches - 2 - group) * obs // CHUNK)

        @pl.loop(group, group + GROUP, step=2)
        def _(turn, later=later):
            assimilate(turn, 0, later)
            assimilate(turn + 1, 1, later)

    for k in range(own_tiles):
        span = slice(k * LANES, (k + 1) * LANES)
        anom_out[pl.ds(k, members, stride=own_tiles), :] = own_state[:members, span]
        mean_out[k : k + 1, :] = -own_state[members : members + 1, span]


def local(anomalies, state_mean, obs_value, obs_cell, owner, order, root_inv, gain_inv):
    members, lon_dev, lat_dev, levels = anomalies.shape
    batches, quarter = obs_value.shape
    obs = obs_cell.shape[1]
    blocks = lon_dev * lat_dev
    own_cells = blocks * levels
    slabs = lax.axis_size("gx")
    bands = lax.axis_size("gy")
    rows = -(-(members + 1) // 8) * 8
    tiles = batches * obs // LANES

    smem = pl.BlockSpec(memory_space=pltpu.SMEM)
    vmem = pl.BlockSpec(memory_space=pltpu.VMEM)
    pairs = batches // 2
    piece = jax.ShapeDtypeStruct((rows, pairs // 2 * LANES), F32)
    own, keep, send = pl.pallas_call(
        functools.partial(gather_kernel, (members, blocks, quarter, pairs)),
        out_shape=(jax.ShapeDtypeStruct((rows, own_cells), F32), piece, piece),
        in_specs=[smem, smem, vmem, vmem, vmem, vmem],
        out_specs=(vmem, vmem, vmem),
        scratch_shapes=[pltpu.VMEM((3 * rows, own_cells), BF16)],
        name="gather_observations",
        compiler_params=pltpu.CompilerParams(vmem_limit_bytes=GATHER_BYTES),
    )(
        order,
        owner,
        obs_cell,
        anomalies.reshape(members * blocks, levels),
        state_mean.reshape(blocks, levels),
        obs_value,
    )

    packed = pl.pallas_call(
        pack_kernel,
        out_shape=jax.ShapeDtypeStruct(
            (2 * (batches // 2 + batches // 4), quarter, LANES), F32
        ),
        in_specs=[vmem, vmem],
        out_specs=vmem,
        name="pack_matrices",
        compiler_params=pltpu.CompilerParams(vmem_limit_bytes=GATHER_BYTES),
    )(root_inv, gain_inv)
    across = swapped(packed, "gy", 2)
    partners = [swapped(root_inv, "gy", 1), swapped(gain_inv, "gy", 1)]

    mine = keep + swapped(send, "gx", 1)
    mask = 2
    while mask < slabs:
        mine = mine + swapped(mine, "gx", mask)
        mask *= 2
    other = swapped(mine, "gx", 1)
    chip = [mine, other, swapped(mine, "gy", 2), swapped(other, "gy", 2)]
    pieces = chip + [swapped(part, "gy", 1) for part in chip]

    dims = (members, lon_dev, lat_dev, quarter, batches, slabs, bands)
    post, post_mean = pl.pallas_call(
        functools.partial(chain_kernel, dims),
        out_shape=(
            jax.ShapeDtypeStruct((members * blocks, levels), F32),
            jax.ShapeDtypeStruct((blocks, levels), F32),
        ),
        in_specs=[smem, smem] + [vmem] * 16,
        out_specs=(vmem, vmem),
        scratch_shapes=[
            pltpu.VMEM((rows, batches * obs), F32),
            pltpu.VMEM((rows, own_cells), F32),
            pltpu.VMEM((tiles, LANES), F32),
            pltpu.VMEM((tiles, LANES), F32),
            pltpu.VMEM((tiles, LANES), F32),
            pltpu.VMEM((2, tiles, LANES), F32),
            pltpu.VMEM((2, tiles, LANES), F32),
            pltpu.VMEM((2, obs, obs), BF16),
            pltpu.VMEM((2, 2 * (-(-rows // 16) * 16), obs), BF16),
            pltpu.VMEM((2, obs, LANES), F32),
            pltpu.VMEM((2, obs, LANES), F32),
            pltpu.VMEM((2, obs, LANES), F32),
            pltpu.VMEM((2, obs, LANES), F32),
        ],
        name="observation_recursion",
        compiler_params=pltpu.CompilerParams(
            vmem_limit_bytes=CHAIN_BYTES
        ),
    )(
        order,
        owner,
        obs_cell,
        own,
        *pieces,
        root_inv,
        gain_inv,
        *partners,
        across,
        swapped(across, "gy", 1),
    )
    return (
        post.reshape(members, lon_dev, lat_dev, levels),
        post_mean.reshape(lon_dev, lat_dev, levels),
    )


def solution(mesh):
    return jax.shard_map(
        local,
        mesh=mesh,
        in_specs=(
            P(None, "gx", "gy", None),
            P("gx", "gy", None),
            P(None, "gy"),
            P(),
            P(),
            P(),
            P(None, "gy", None),
            P(None, "gy", None),
        ),
        out_specs=(P(None, "gx", "gy", None), P("gx", "gy", None)),
        check_vma=False,
    )
```

```python
import functools
import jax
import jax.numpy as jnp
from jax import lax
from jax.experimental import pallas as pl
from jax.experimental.pallas import tpu as pltpu
from jax.sharding import PartitionSpec as P

REACH = 3
LANES = 128
CHUNK = 512
GROUP = 4
LAG = 2
LATE_LAG = 4
LOOPED = 4
DEPTH = 1
HOIST = 16
GATHER_BYTES = 12 * 2**20
CHAIN_BYTES = 20 * 2**20
STRIP = 16
F32 = jnp.float32
BF16 = jnp.bfloat16


def swapped(value, axis, mask):
    count = lax.axis_size(axis)
    return lax.ppermute(value, axis, [(source, source ^ mask) for source in range(count)])


def split(value):
    high = value.astype(BF16).astype(F32)
    return high, value - high


def dot(left, right):
    return jnp.dot(left, right, preferred_element_type=F32)


def gather_kernel(
    dims, order, owner, cells, anom, mean, obs, own_out, keep_out, send_out, parts
):
    members, blocks, quarter, pairs = dims
    rows = own_out.shape[0]
    column, band = lax.axis_index("gx"), lax.axis_index("gy")
    half = lax.rem(column, 2)
    for k in range(blocks):
        block = anom[pl.ds(k, members, stride=blocks), :]
        extra = jnp.concatenate(
            [-mean[k : k + 1, :], jnp.zeros((rows - members - 1, LANES), F32)], axis=0
        )
        block = jnp.concatenate([block, extra], axis=0)
        own_out[:, k * LANES : (k + 1) * LANES] = block
        high, rest = split(block)
        mid, low = split(rest)
        stack = jnp.concatenate([high, mid, low], axis=0)
        parts[:, k * LANES : (k + 1) * LANES] = stack.astype(BF16)
    lane = lax.broadcasted_iota(jnp.int32, (1, LANES), 1)
    first = lane < quarter
    total = cells.shape[1]
    shift = lax.rem(total - band * quarter, total)

    def ids_of(pair):
        even, odd = order[2 * pair], order[2 * pair + 1]
        row_even = pltpu.roll(cells[pl.ds(even, 1), :], shift, 1)[:, :LANES]
        row_odd = pltpu.roll(cells[pl.ds(odd, 1), :], lax.rem(shift + quarter, total), 1)
        row_odd = row_odd[:, :LANES]
        here_even = owner[even] == column
        here_odd = owner[odd] == column
        mine = jnp.where(first, here_even.astype(jnp.int32), here_odd.astype(jnp.int32))
        ids = jnp.where(mine > 0, jnp.where(first, row_even, row_odd), -1)
        seen = jnp.concatenate([obs[pl.ds(even, 1), :], obs[pl.ds(odd, 1), :]], axis=1)
        seen = jnp.where(mine > 0, seen, 0.0)
        return ids, seen, jnp.logical_or(here_even, here_odd)

    tail = pairs // 2 * members

    def put(out, slot, columns, mean_row):
        for k in range(2):
            lanes = slice(k * LANES, (k + 1) * LANES)
            first_row = (slot + k) * members
            out[first_row : first_row + members, :] = columns[:, lanes]
            out[tail + slot + k : tail + slot + k + 1, :] = mean_row[:, lanes]

    for out, which in ((keep_out, half), (send_out, 1 - half)):
        out[tail:, :] = jnp.zeros((out.shape[0] - tail, LANES), F32)
        for slot in range(0, pairs // 2, 2):
            pair = which * (pairs // 2) + slot
            ids_a, seen_a, any_a = ids_of(pair)
            ids_b, seen_b, any_b = ids_of(pair + 1)
            ids = jnp.concatenate([ids_a, ids_b], axis=1)
            seen = jnp.concatenate([seen_a, seen_b], axis=1)
            span = slot
            busy = jnp.logical_or(any_a, any_b)

            @pl.when(busy)
            def _(out=out, ids=ids, seen=seen, span=span):
                total_cells = parts.shape[1]
                cell = lax.broadcasted_iota(jnp.int32, (total_cells, 2 * LANES), 0)
                hot = jnp.where(cell == ids, 1.0, 0.0).astype(BF16)
                found = dot(parts[...], hot)
                value = found[:rows] + found[rows : 2 * rows] + found[2 * rows :]
                put(out, span, value[:members], value[members : members + 1] + seen)

            @pl.when(jnp.logical_not(busy))
            def _(out=out, span=span):
                empty = jnp.zeros((members, 2 * LANES), F32)
                put(out, span, empty, empty[:1])


def pack_kernel(root, gain, out):
    batches, quarter = root.shape[:2]
    band = lax.axis_index("gy")
    core, chip = lax.rem(band, 2), lax.div(band, 2)
    near = pl.ds(pl.multiple_of(chip * LANES, LANES), LANES)
    first = lax.broadcasted_iota(jnp.int32, (1, LANES), 1) < quarter
    stride = batches // 2 + batches // 4
    for kind, source in enumerate((root, gain)):

        def joined(left, right, own_half_is_left):
            left = jnp.where(own_half_is_left, left, pltpu.roll(left, quarter, 1))
            right = jnp.where(own_half_is_left, pltpu.roll(right, quarter, 1), right)
            return jnp.where(first, left, right)

        for k in range(batches // 2):
            out[kind * stride + k] = joined(
                source[2 * k, :, near], source[2 * k + 1, :, near], core == 0
            )
        for k in range(batches // 4):
            out[kind * stride + batches // 2 + k] = joined(
                source[4 * k + core, :, near], source[4 * k + 2 + core, :, near], core != 0
            )


def chain_kernel(
    dims,
    order,
    owner,
    cells,
    own,
    *refs,
):
    members, lon_dev, lat_dev, quarter, batches, slabs, bands = dims
    pieces = refs[:8]
    locals_, partners, across, relayed = refs[8:10], refs[10:12], refs[12], refs[13]
    anom_out, mean_out = refs[14:16]
    state, own_state, lon_at, lat_at, slope_at, near, far, zcat, wcat = refs[16:25]
    lat_of, rise_of, bit_of, own_taper = refs[25:]
    rows = state.shape[0]
    own_cells = own.shape[1]
    own_tiles = own_cells // LANES
    obs = bands * quarter
    column, band = lax.axis_index("gx"), lax.axis_index("gy")
    core = lax.rem(band, 2)
    chip = lax.div(band, 2)
    lat_total = float(bands * lat_dev)
    lon_total = float(slabs * lon_dev)
    reach_span = REACH * lon_dev + 1.0

    own_state[...] = own[...]
    lane = lax.broadcasted_iota(jnp.int32, (1, LANES), 1)
    first = lane < quarter
    low_core = jnp.where(first, 1, 0) * jnp.where(core == 0, 1, 0) + jnp.where(
        first, 0, 1
    ) * jnp.where(core == 0, 0, 1)
    from_self = low_core > 0
    half_pairs = batches // 4
    is_mean = lax.broadcasted_iota(jnp.int32, (rows - members, LANES), 0) == 0

    def tile_of(piece, k):
        at = half_pairs * members + k
        mean_row = jnp.where(is_mean, piece[at : at + 1, :], 0.0)
        return jnp.concatenate([piece[k * members : (k + 1) * members, :], mean_row], axis=0)

    half = lax.rem(column, 2)
    for which in range(2):
        pair_base = (half if which == 0 else 1 - half) * half_pairs
        for side in range(2):
            mine = pieces[2 * side + which]
            theirs = pieces[4 + 2 * side + which]
            for k in range(half_pairs):
                a, b = tile_of(mine, k), tile_of(theirs, k)
                a_roll, b_roll = pltpu.roll(a, quarter, 1), pltpu.roll(b, quarter, 1)
                a_first, b_first = (
                    jnp.where(core == 0, a, a_roll),
                    jnp.where(core == 0, b_roll, b),
                )
                a_last, b_last = (
                    jnp.where(core == 0, a_roll, a),
                    jnp.where(core == 0, b, b_roll),
                )
                turn = 2 * (pair_base + k)
                for step, (x, y) in enumerate(((a_first, b_first), (a_last, b_last))):
                    at = (batches - 1 - turn - step) * obs + side * LANES
                    at = pl.multiple_of(at, LANES)
                    state[:, pl.ds(at, LANES)] = jnp.where(from_self, x, y)

    side_sign = jnp.where(chip > 0, 1.0, -1.0)

    @pl.loop(0, batches)
    def _(turn):
        b = order[turn]
        cells_row = cells[pl.ds(b, 1), :]
        for side in range(2):
            group = chip if side == 0 else 1 - chip
            cell = jnp.where(group == 0, cells_row[:, :LANES], cells_row[:, LANES:])
            level_band = lax.shift_right_logical(cell, (LANES - 1).bit_length())
            lat = group * 2 + jnp.where(first, 0, 1)
            lat = lat * lat_dev + lax.rem(level_band, lat_dev)
            lon = owner[b] * lon_dev + lax.div(level_band, lat_dev)
            row = (batches - 1 - turn) * 2 + side
            lon_at[pl.ds(row, 1), :] = lon.astype(F32)
            lat = lat.astype(F32) / lat_total
            lat_at[pl.ds(row, 1), :] = lat
            slope_at[pl.ds(row, 1), :] = lat * (-side_sign if side == 0 else side_sign)

    own_lon = (column * lon_dev + lane // lat_dev).astype(F32)
    own_lat = (band * lat_dev + lane % lat_dev).astype(F32) / lat_total

    def lon_factor(places, lon):
        gap = jnp.abs(places - lon)
        gap = jnp.minimum(gap, lon_total - gap)
        return jnp.maximum(0.0, 1.0 - gap / reach_span)

    near_cols = pl.ds(pl.multiple_of(chip * LANES, LANES), LANES)
    far_cols = pl.ds(pl.multiple_of((1 - chip) * LANES, LANES), LANES)
    stride = batches // 2 + batches // 4

    def by_core(mine, theirs):
        is_even = core == 0
        return jnp.where(is_even, mine, theirs), jnp.where(is_even, theirs, mine)

    def symmetric(kind, b):
        mine, theirs = locals_[kind], partners[kind]
        blocks = [
            jnp.concatenate(by_core(mine[b, :, cols], theirs[b, :, cols]), axis=0)
            for cols in (near_cols, far_cols)
        ]
        pair, odd = lax.div(b, 2), lax.rem(b, 2)
        at = kind * stride + pair
        even_tile, odd_tile = by_core(across[at], relayed[at])
        even_even = jnp.where(odd == 0, even_tile, pltpu.roll(even_tile, quarter, 1))
        odd_odd = jnp.where(odd == 0, pltpu.roll(odd_tile, quarter, 1), odd_tile)
        at = kind * stride + batches // 2 + lax.div(pair, 2)
        cross = jnp.where(odd == core, across[at], relayed[at])
        turned = pltpu.roll(cross, quarter, 1)
        is_left = lax.rem(pair, 2) == 0
        cross, turned = jnp.where(is_left, cross, turned), jnp.where(is_left, turned, cross)
        cross = jnp.where(first, cross, turned)
        flipped = jnp.concatenate([cross, cross], axis=0).T[:quarter]
        even_odd = jnp.where(odd == 0, cross, flipped)
        odd_even = jnp.where(odd == 0, flipped, cross)
        corner = jnp.concatenate(
            [jnp.where(first, even_even, even_odd), jnp.where(first, odd_even, odd_odd)], axis=0
        )
        whole = jnp.concatenate(
            [
                jnp.concatenate(blocks, axis=1),
                jnp.concatenate([blocks[1].T, corner], axis=1),
            ],
            axis=0,
        )
        high, low = split(whole)
        return high.astype(BF16), low.astype(BF16)

    def thrice(high, low, right_high, right_low):
        count = high.shape[0]
        both = dot(jnp.concatenate([high, low], axis=0).astype(BF16), right_high)
        return both[:count] + both[count:] + dot(high.astype(BF16), right_low)

    def prepare(turn, p, z):
        z_high, z_low = split(z[:members])
        pad = jnp.zeros((obs - 3 * members, obs), F32)
        zcat[p] = jnp.concatenate([z_high, z_high, z_low, pad], axis=0).T.astype(BF16)
        d_high, d_low = split(z[members:])
        v = thrice(z_high, z_low, *symmetric(0, order[turn]))
        u = thrice(d_high, d_low, *symmetric(1, order[turn]))
        w = jnp.concatenate([v, u], axis=0) * (1.0 / (members - 1.0))
        w_high, w_low = split(w)
        fill = jnp.zeros((wcat.shape[1] // 2 - rows, obs), F32)
        wcat[p] = jnp.concatenate([w_high, fill, w_low, fill], axis=0).astype(BF16)

        base = (owner[order[turn]] * lon_dev).astype(F32)
        near[p] = lon_factor(lon_at[...], base)
        far[p] = lon_factor(lon_at[...], base + 1.0)
        for side in range(2):
            row = (batches - 1 - turn) * 2 + side
            lat_row = jnp.broadcast_to(lat_at[pl.ds(row, 1), :], (LANES, LANES))
            bit_row = jnp.broadcast_to(lon_at[pl.ds(row, 1), :] - base, (LANES, LANES))
            span = slice(side * LANES, (side + 1) * LANES)
            lat_column = lat_row.T
            lat_of[p, span, :] = lat_column
            rise_of[p, span, :] = 1.0 - lat_column * (side_sign if side == 0 else -side_sign)
            bit_of[p, span, :] = bit_row.T
        own_near = lon_factor(own_lon, base)
        own_far = lon_factor(own_lon, base + 1.0)
        lat_part = 1.0 - jnp.abs(lat_of[p] - own_lat)
        own_taper[p] = lat_part * jnp.where(bit_of[p] > 0.5, own_far, own_near)

    def covariance(p, start, width, kind, row):
        source = state if kind == "obs" else own_state
        now = source[:members, pl.ds(start, width)]
        high, low = split(now)
        zeros = jnp.zeros((obs - 3 * members, width), F32)
        right = jnp.concatenate([high, low, high, zeros], axis=0).astype(BF16)
        return dot(zcat[p], right)

    def updated(p, start, width, kind, row, cov):
        tiles = range(width // LANES)
        if kind == "obs":
            near_row = [near[p, pl.ds(row + k, 1), :] for k in tiles]
            far_row = [far[p, pl.ds(row + k, 1), :] for k in tiles]
            lat_row = [lat_at[pl.ds(row + k, 1), :] for k in tiles]
            slope_row = [slope_at[pl.ds(row + k, 1), :] for k in tiles]
        highs, lows = [], []
        for j in range(0, obs, STRIP):
            span = slice(j, j + STRIP)
            if kind == "obs":
                lat, rise = lat_of[p, span, :], rise_of[p, span, :]
                is_far = bit_of[p, span, :] > 0.5
            strip = []
            for k in tiles:
                if kind == "obs":
                    if (j < 2 * quarter) == (k % 2 == 0):
                        lat_part = 1.0 - jnp.abs(lat - lat_row[k])
                    else:
                        lat_part = rise + slope_row[k]
                    factor = lat_part * jnp.where(is_far, far_row[k], near_row[k])
                else:
                    factor = jnp.broadcast_to(
                        own_taper[p, span, row + k : row + k + 1], (STRIP, LANES)
                    )
                strip.append(cov[span, k * LANES : (k + 1) * LANES] * factor)
            strip = jnp.concatenate(strip, axis=1)
            high = strip.astype(BF16)
            highs.append(high)
            lows.append((strip - high.astype(F32)).astype(BF16))
        g_high = jnp.concatenate(highs, axis=0)
        g_low = jnp.concatenate(lows, axis=0)
        deep = wcat.shape[1] // 2
        both = dot(wcat[p], g_high)
        change = both[:deep] + both[deep:] + dot(wcat[p, :deep, :], g_low)
        source = state if kind == "obs" else own_state
        return source[:, pl.ds(start, width)] - change[:rows]

    wide = CHUNK // LANES

    def assimilate(turn, p, later):
        work = []
        last = isinstance(turn, int) and turn + 1 == batches
        if not last:
            coming = turn + 1
            row = (batches - 1 - coming) * 2
            at = row * LANES if isinstance(row, int) else pl.multiple_of(row * LANES, obs)
            work.append((at, obs, "obs", row))
        for c in reversed(range(later)):
            work.append((c * CHUNK, CHUNK, "obs", c * wide))
        for c in range(own_cells // CHUNK):
            work.append((c * CHUNK, CHUNK, "own", c * wide))
        ready = [covariance(p, *item) for item in work[:DEPTH]]
        z = None
        for i, item in enumerate(work):
            if i + DEPTH < len(work):
                ready.append(covariance(p, *work[i + DEPTH]))
            value = updated(p, *item, ready[i])
            if i == 0 and not last:
                z = value
            else:
                target = state if item[2] == "obs" else own_state
                target[:, pl.ds(item[0], item[1])] = value
            if i == (LAG if later > 4 else LATE_LAG) and not last:
                prepare(coming, 1 - p, z)

    first_at = (batches - 1) * obs
    prepare(jnp.int32(0), 0, state[:, first_at : first_at + obs])
    for group in range(0, batches, GROUP):
        if group >= LOOPED:
            for turn in range(group, group + GROUP):
                assimilate(turn, turn % 2, max(0, -(-(batches - 2 - turn) * obs // CHUNK)))
            continue
        later = -(-(batches - 2 - group) * obs // CHUNK)

        @pl.loop(group, group + GROUP, step=2)
        def _(turn, later=later):
            assimilate(turn, 0, later)
            assimilate(turn + 1, 1, later)

    for k in range(own_tiles):
        span = slice(k * LANES, (k + 1) * LANES)
        anom_out[pl.ds(k, members, stride=own_tiles), :] = own_state[:members, span]
        mean_out[k : k + 1, :] = -own_state[members : members + 1, span]


def local(anomalies, state_mean, obs_value, obs_cell, owner, order, root_inv, gain_inv):
    members, lon_dev, lat_dev, levels = anomalies.shape
    batches, quarter = obs_value.shape
    obs = obs_cell.shape[1]
    blocks = lon_dev * lat_dev
    own_cells = blocks * levels
    slabs = lax.axis_size("gx")
    bands = lax.axis_size("gy")
    rows = -(-(members + 1) // 8) * 8
    tiles = batches * obs // LANES

    smem = pl.BlockSpec(memory_space=pltpu.SMEM)
    vmem = pl.BlockSpec(memory_space=pltpu.VMEM)
    pairs = batches // 2
    piece_rows = pairs // 2 * members + -(-pairs // 16) * 8
    piece = jax.ShapeDtypeStruct((piece_rows, LANES), F32)
    own, keep, send = pl.pallas_call(
        functools.partial(gather_kernel, (members, blocks, quarter, pairs)),
        out_shape=(jax.ShapeDtypeStruct((rows, own_cells), F32), piece, piece),
        in_specs=[smem, smem, vmem, vmem, vmem, vmem],
        out_specs=(vmem, vmem, vmem),
        scratch_shapes=[pltpu.VMEM((3 * rows, own_cells), BF16)],
        name="gather_observations",
        compiler_params=pltpu.CompilerParams(vmem_limit_bytes=GATHER_BYTES),
    )(
        order,
        owner,
        obs_cell,
        anomalies.reshape(members * blocks, levels),
        state_mean.reshape(blocks, levels),
        obs_value,
    )

    packed = pl.pallas_call(
        pack_kernel,
        out_shape=jax.ShapeDtypeStruct(
            (2 * (batches // 2 + batches // 4), quarter, LANES), F32
        ),
        in_specs=[vmem, vmem],
        out_specs=vmem,
        name="pack_matrices",
        compiler_params=pltpu.CompilerParams(vmem_limit_bytes=GATHER_BYTES),
    )(root_inv, gain_inv)
    across = swapped(packed, "gy", 2)
    partners = [swapped(root_inv, "gy", 1), swapped(gain_inv, "gy", 1)]

    mine = keep + swapped(send, "gx", 1)
    mask = 2
    while mask < slabs:
        mine = mine + swapped(mine, "gx", mask)
        mask *= 2
    other = swapped(mine, "gx", 1)
    chip = [mine, other, swapped(mine, "gy", 2), swapped(other, "gy", 2)]
    pieces = chip + [swapped(part, "gy", 1) for part in chip]

    dims = (members, lon_dev, lat_dev, quarter, batches, slabs, bands)
    post, post_mean = pl.pallas_call(
        functools.partial(chain_kernel, dims),
        out_shape=(
            jax.ShapeDtypeStruct((members * blocks, levels), F32),
            jax.ShapeDtypeStruct((blocks, levels), F32),
        ),
        in_specs=[smem, smem] + [vmem] * 16,
        out_specs=(vmem, vmem),
        scratch_shapes=[
            pltpu.VMEM((rows, batches * obs), F32),
            pltpu.VMEM((rows, own_cells), F32),
            pltpu.VMEM((tiles, LANES), F32),
            pltpu.VMEM((tiles, LANES), F32),
            pltpu.VMEM((tiles, LANES), F32),
            pltpu.VMEM((2, tiles, LANES), F32),
            pltpu.VMEM((2, tiles, LANES), F32),
            pltpu.VMEM((2, obs, obs), BF16),
            pltpu.VMEM((2, 2 * (-(-rows // 16) * 16), obs), BF16),
            pltpu.VMEM((2, obs, LANES), F32),
            pltpu.VMEM((2, obs, LANES), F32),
            pltpu.VMEM((2, obs, LANES), F32),
            pltpu.VMEM((2, obs, LANES), F32),
        ],
        name="observation_recursion",
        compiler_params=pltpu.CompilerParams(
            vmem_limit_bytes=CHAIN_BYTES
        ),
    )(
        order,
        owner,
        obs_cell,
        own,
        *pieces,
        root_inv,
        gain_inv,
        *partners,
        across,
        swapped(across, "gy", 1),
    )
    return (
        post.reshape(members, lon_dev, lat_dev, levels),
        post_mean.reshape(lon_dev, lat_dev, levels),
    )


def solution(mesh):
    return jax.shard_map(
        local,
        mesh=mesh,
        in_specs=(
            P(None, "gx", "gy", None),
            P("gx", "gy", None),
            P(None, "gy"),
            P(),
            P(),
            P(),
            P(None, "gy", None),
            P(None, "gy", None),
        ),
        out_specs=(P(None, "gx", "gy", None), P("gx", "gy", None)),
        check_vma=False,
    )
```
